16 devices in a mesh: dp: 2 (over y, z), ep: 8 (over x, core).
Axes of the slice: x: 4, y: 2, z: 1, core: 2. Of those that a mesh axis runs over, the one named last changes fastest.
The devices are a block of a 4x4x8 slice.
Arguments:
- tokens: bfloat16 [16, 2048, 2048], P(('dp', 'ep')), parts along dimension 0
- w_gate: bfloat16 [2048, 128], replicated
- expert_ids: int32 [16, 2048, 2], P(('dp', 'ep')), parts along dimension 0
- keep_second: int32 [16, 2048], P(('dp', 'ep')), parts along dimension 0
- w_in: bfloat16 [128, 2048, 768], P('ep')
- w_out: bfloat16 [128, 768, 2048], P('ep')
Outputs:
- output: bfloat16 [16, 2048, 2048], P(('dp', 'ep')), parts along dimension 0
There are 2 independent parts. The reference program is written for one: setup_inputs(seed, part) draws one part's arguments, and reference() takes and returns one part's arrays. A program takes and returns all parts, laid end to end along the dimension named above; an argument that names none is the same for every part.
All inputs are finite; a program needn't handle non-finite values.
Results may differ from the reference program's by a relative error of at most 0.001.
Values are sent between devices in bfloat16 or wider.
A program may use at most 768 MiB of HBM per device.

```python
import functools
import jax
import jax.numpy as jnp
from jax import lax

GROUPS = 8
TOKENS = 2048
MODEL_DIM = 2048
HIDDEN = 768
EXPERTS = 128
CAPACITY = 2 * TOKENS // EXPERTS


def draw_routing(route_key):
    k_cover, k_raw, k_shift, k_second, k_keep = jax.random.split(route_key, 5)
    cover_keys = jax.random.split(k_cover, GROUPS)
    cover_ids = jax.vmap(functools.partial(jax.random.permutation, x=EXPERTS))(cover_keys)
    hot_shift = jax.random.randint(k_shift, (), 0, EXPERTS)
    raw_ids = jax.random.randint(k_raw, (GROUPS, TOKENS - EXPERTS), 0, EXPERTS + EXPERTS // 2)
    rest_ids = (raw_ids % EXPERTS + hot_shift) % EXPERTS
    first_ids = jnp.concatenate([cover_ids.astype(jnp.int32), rest_ids.astype(jnp.int32)], axis=1)
    second_ids = (first_ids + jax.random.randint(k_second, (GROUPS, TOKENS), 1, EXPERTS)) % EXPERTS
    keep_second = (jax.random.randint(k_keep, (GROUPS, TOKENS), 0, 10) < 9).astype(jnp.int32)
    expert_ids = jnp.stack([first_ids, second_ids], axis=-1).astype(jnp.int32)
    return expert_ids, keep_second


def setup_inputs(seed: int = 0, part: int = 0) -> dict:
    shared_key, parts_key = jax.random.split(jax.random.key(seed))
    part_key = jax.random.fold_in(parts_key, part)
    k_tokens, k_route = jax.random.split(part_key)
    k_gate, k_in, k_out = jax.random.split(shared_key, 3)
    tokens = jax.random.normal(k_tokens, (GROUPS, TOKENS, MODEL_DIM), jnp.float32).astype(jnp.bfloat16)
    expert_ids, keep_second = draw_routing(k_route)
    w_gate = (jax.random.normal(k_gate, (MODEL_DIM, EXPERTS), jnp.float32) * MODEL_DIM ** -0.5).astype(jnp.bfloat16)
    w_in = (jax.random.normal(k_in, (EXPERTS, MODEL_DIM, HIDDEN), jnp.float32) * MODEL_DIM ** -0.5).astype(jnp.bfloat16)
    w_out = (jax.random.normal(k_out, (EXPERTS, HIDDEN, MODEL_DIM), jnp.float32) * (2.0 / HIDDEN) ** 0.5).astype(jnp.bfloat16)
    return {"tokens": tokens, "w_gate": w_gate, "expert_ids": expert_ids, "keep_second": keep_second, "w_in": w_in, "w_out": w_out}


def group_routing(group_tok, group_ids, group_keep, w_gate):
    logits = jnp.dot(group_tok, w_gate, preferred_element_type=jnp.float32)
    gate_probs = jax.nn.softmax(logits, axis=-1)
    first_hot = jax.nn.one_hot(group_ids[:, 0], EXPERTS, dtype=jnp.int32)
    second_hot = jax.nn.one_hot(group_ids[:, 1], EXPERTS, dtype=jnp.int32) * group_keep[:, None]
    gate_first = jnp.sum(gate_probs * first_hot, axis=-1)
    gate_second = jnp.sum(gate_probs * second_hot, axis=-1)
    gate_total = gate_first + gate_second
    gate_first = gate_first / gate_total
    gate_second = gate_second / gate_total
    pos_first = jnp.sum((jnp.cumsum(first_hot, axis=0) - first_hot) * first_hot, axis=-1)
    second_base = jnp.cumsum(second_hot, axis=0) - second_hot + jnp.sum(first_hot, axis=0)[None, :]
    pos_second = jnp.sum(second_base * second_hot, axis=-1)
    slot_first = first_hot[:, :, None] * jax.nn.one_hot(pos_first, CAPACITY, dtype=jnp.float32)[:, None, :]
    slot_second = second_hot[:, :, None] * jax.nn.one_hot(pos_second, CAPACITY, dtype=jnp.float32)[:, None, :]
    dispatch = slot_first + slot_second
    combine = (gate_first[:, None, None] * slot_first + gate_second[:, None, None] * slot_second).astype(jnp.bfloat16)
    return dispatch, combine


def reference(tokens, w_gate, expert_ids, keep_second, w_in, w_out):
    def dispatch_group(operands):
        group_tok, group_ids, group_keep = operands
        dispatch, _ = group_routing(group_tok, group_ids, group_keep, w_gate)
        sent_rows = jnp.einsum("sec,sm->ecm", dispatch.astype(jnp.float32), group_tok.astype(jnp.float32))
        return sent_rows.astype(jnp.bfloat16)

    expert_in = lax.map(dispatch_group, (tokens, expert_ids, keep_second))
    expert_in = jnp.transpose(expert_in, (1, 0, 2, 3))

    def expert_ffn(operands):
        rows_in, w_first, w_second = operands
        flat_rows = rows_in.reshape(GROUPS * CAPACITY, MODEL_DIM)
        hidden = jax.nn.relu(jnp.dot(flat_rows, w_first, preferred_element_type=jnp.float32)).astype(jnp.bfloat16)
        rows_out = jnp.dot(hidden, w_second, preferred_element_type=jnp.float32).astype(jnp.bfloat16)
        return rows_out.reshape(GROUPS, CAPACITY, MODEL_DIM)

    expert_out = lax.map(expert_ffn, (expert_in, w_in, w_out))
    expert_out = jnp.transpose(expert_out, (1, 0, 2, 3))

    def combine_group(operands):
        group_tok, group_ids, group_keep, rows_back = operands
        _, combine = group_routing(group_tok, group_ids, group_keep, w_gate)
        mixed_rows = jnp.einsum("sec,ecm->sm", combine.astype(jnp.float32), rows_back.astype(jnp.float32))
        return mixed_rows.astype(jnp.bfloat16)

    return lax.map(combine_group, (tokens, expert_ids, keep_second, expert_out))
```

```python
import functools

import jax
import jax.numpy as jnp
from jax import lax
from jax.experimental import pallas as pl
from jax.experimental.pallas import tpu as pltpu
from jax.sharding import PartitionSpec as P

MESH = pl.DeviceIdType.MESH
LAG = 3
TILE = 256


def ring_offsets(chip_count):
    near = sorted(range(1, chip_count), key=lambda d: min(d, chip_count - d))
    return near


def moe_kernel(
    n, sizes, ids_ref, keep_ref, x_hbm, wg_ref, win_hbm, wout_hbm, out_hbm,
    x_v, acc, win_v, wout_v, fsend, frecv, ysend, yrecv, dmat, hid, crow, colb,
    x_sem, win_sem, wout_sem, fs_sem, fr_sem, ys_sem, yr_sem, out_sem,
):
    tokens, model, hidden, experts, local, capacity = sizes
    rows = n * capacity
    fslots, yslots = frecv.shape[0], yrecv.shape[0]
    shift = (local - 1).bit_length()
    blocks = tokens // TILE
    me = lax.axis_index("ep")

    x_copy = pltpu.make_async_copy(x_hbm.at[0], x_v, x_sem)

    def weight_copies(k):
        b = lax.rem(k, 2)
        return (
            pltpu.make_async_copy(win_hbm.at[k], win_v.at[b], win_sem.at[b]),
            pltpu.make_async_copy(wout_hbm.at[k], wout_v.at[b], wout_sem.at[b]),
        )

    def owner_rows(d):
        return pl.ds(pl.multiple_of(d * capacity, capacity), capacity)

    cores = 2 if n % 2 == 0 else 1
    chips = n // cores
    my_chip, my_core = me // cores, lax.rem(me, cores)
    targets = []
    for dist in ring_offsets(chips) + [0]:
        for c in range(cores):
            if dist == 0 and c == 0:
                continue
            targets.append(lax.rem(my_chip + dist, chips) * cores + lax.rem(my_core + c, cores))

    def send(src, src_slot, dst, dst_slot, s_sem, r_sem):
        for d in targets:
            pltpu.make_async_remote_copy(
                src_ref=src.at[src_slot, owner_rows(d)],
                dst_ref=dst.at[dst_slot, owner_rows(me)],
                send_sem=s_sem.at[src_slot],
                recv_sem=r_sem.at[dst_slot],
                device_id={"ep": d},
                device_id_type=MESH,
            ).start()

    def all_peers(src, src_slot, dst, dst_slot, s_sem, r_sem):
        part = pl.ds(0, (n - 1) * capacity)
        return pltpu.make_async_remote_copy(
            src_ref=src.at[src_slot, part],
            dst_ref=dst.at[dst_slot, part],
            send_sem=s_sem.at[src_slot],
            recv_sem=r_sem.at[dst_slot],
            device_id={"ep": me},
            device_id_type=MESH,
        )

    def fwd_args(k):
        return (fsend, lax.rem(k, 2), frecv, lax.rem(k, fslots), fs_sem, fr_sem)

    def back_args(k):
        return (ysend, lax.rem(k, 2), yrecv, lax.rem(k, yslots), ys_sem, yr_sem)

    def keep_own(src, src_slot, dst, dst_slot, *_):
        dst[dst_slot, owner_rows(me), :] = src[src_slot, owner_rows(me), :]

    def hot(blk, expert_row):
        return lax.broadcasted_iota(jnp.int32, (experts, TILE), 0) == expert_row

    def load_ids(b):
        cols = pl.ds(b * TILE, TILE)
        return ids_ref[0:1, cols], ids_ref[1:2, cols], keep_ref[0:1, cols] == 1

    def route():
        count = jnp.zeros((experts, TILE), jnp.float32)
        for b in range(blocks):
            i1, _, _ = load_ids(b)
            count = count + hot(b, i1).astype(jnp.float32)
        base1 = jnp.zeros((experts, 1), jnp.float32)
        base2 = jnp.sum(count, axis=1, keepdims=True)
        before = (
            lax.broadcasted_iota(jnp.int32, (TILE, TILE), 0) < lax.broadcasted_iota(jnp.int32, (TILE, TILE), 1)
        ).astype(jnp.bfloat16)
        for b in range(blocks):
            i1, i2, k2 = load_ids(b)
            hot1 = hot(b, i1).astype(jnp.float32)
            hot2 = jnp.where(k2, hot(b, i2).astype(jnp.float32), 0.0)
            ahead1 = jnp.dot(hot1.astype(jnp.bfloat16), before, preferred_element_type=jnp.float32) + base1
            ahead2 = jnp.dot(hot2.astype(jnp.bfloat16), before, preferred_element_type=jnp.float32) + base2
            base1 = base1 + jnp.sum(hot1, axis=1, keepdims=True)
            base2 = base2 + jnp.sum(hot2, axis=1, keepdims=True)
            pos1 = jnp.sum(ahead1 * hot1, axis=0, keepdims=True)
            pos2 = jnp.sum(ahead2 * hot2, axis=0, keepdims=True)

            def code(e, pos, kept):
                home = (e & (local - 1)) * rows + (e >> shift) * capacity
                return jnp.where(kept, home.astype(jnp.float32) + pos, -1.0)

            cols = pl.ds(b * TILE, TILE)
            crow[0:1, cols] = code(i1, pos1, pos1 < capacity)
            crow[1:2, cols] = code(i2, pos2, jnp.logical_and(k2, pos2 < capacity))

    def gates():
        for b in range(blocks):
            cols = pl.ds(b * TILE, TILE)
            i1, i2, k2 = load_ids(b)
            logits = jnp.dot(x_v[cols, :], wg_ref[...], preferred_element_type=jnp.float32).T
            top = jnp.max(logits, axis=0, keepdims=True)
            grown = jnp.exp(logits - top)
            probs = grown / jnp.sum(grown, axis=0, keepdims=True)
            g1 = jnp.sum(jnp.where(hot(b, i1), probs, 0.0), axis=0, keepdims=True)
            g2 = jnp.where(k2, jnp.sum(jnp.where(hot(b, i2), probs, 0.0), axis=0, keepdims=True), 0.0)
            total = g1 + g2
            for q, row in enumerate((crow[0:1, cols], crow[1:2, cols], g1 / total, g2 / total)):
                colb[q, cols, :] = jnp.broadcast_to(row, (128, TILE)).T

    def dispatch(k):
        slot = lax.rem(k, 2)
        base = (k * rows).astype(jnp.float32)
        for b in range(blocks):
            cols = pl.ds(b * TILE, TILE)
            want = lax.broadcasted_iota(jnp.int32, (rows, TILE), 0).astype(jnp.float32)
            c1, c2 = crow[0:1, cols] - base, crow[1:2, cols] - base
            dmat[:, cols] = jnp.where(jnp.logical_or(c1 == want, c2 == want), 1.0, 0.0).astype(jnp.bfloat16)

        @pl.loop(0, model // TILE)
        def _(j):
            cols = pl.ds(pl.multiple_of(j * TILE, TILE), TILE)
            fsend[slot, :, cols] = jnp.dot(
                dmat[...], x_v[:, cols], preferred_element_type=jnp.float32
            ).astype(jnp.bfloat16)

    def experts_ffn(k):
        w, slot, out_slot = lax.rem(k, 2), lax.rem(k, fslots), lax.rem(k, 2)

        @pl.loop(0, hidden // TILE)
        def _(j):
            cols = pl.ds(pl.multiple_of(j * TILE, TILE), TILE)
            h = jnp.dot(frecv[slot], win_v[w, :, cols], preferred_element_type=jnp.float32)
            hid[:, cols] = jnp.maximum(h, 0.0).astype(jnp.bfloat16)

        @pl.loop(0, model // TILE)
        def _(j):
            cols = pl.ds(pl.multiple_of(j * TILE, TILE), TILE)
            y = jnp.dot(hid[...], wout_v[w, :, cols], preferred_element_type=jnp.float32)
            ysend[out_slot, :, cols] = y.astype(jnp.bfloat16)

    def mix_weights(k, toks):
        base = (k * rows).astype(jnp.float32)
        c1, c2 = colb[0, toks, :] - base, colb[1, toks, :] - base
        w1, w2 = colb[2, toks, :], colb[3, toks, :]
        parts = []
        for lane in range(0, rows, 128):
            want = (lax.broadcasted_iota(jnp.int32, (TILE, 128), 1) + lane).astype(jnp.float32)
            parts.append((jnp.where(c1 == want, w1, 0.0) + jnp.where(c2 == want, w2, 0.0)).astype(jnp.bfloat16))
        return jnp.concatenate(parts, axis=1)

    def combine(k, last):
        slot = lax.rem(k, yslots)

        @pl.loop(0, blocks)
        def _(i):
            toks = pl.ds(pl.multiple_of(i * TILE, TILE), TILE)
            mix = mix_weights(k, toks)
            for j in range(0, model, 2 * TILE):
                cols = pl.ds(j, 2 * TILE)
                got = acc[toks, cols] + jnp.dot(mix, yrecv[slot, :, cols], preferred_element_type=jnp.float32)
                if last:
                    x_v[toks, cols] = got.astype(jnp.bfloat16)
                else:
                    acc[toks, cols] = got
            if last:
                pltpu.make_async_copy(x_v.at[toks], out_hbm.at[0, toks], out_sem).start()

    x_copy.start()
    for copy in weight_copies(0):
        copy.start()
    barrier = pltpu.get_barrier_semaphore()
    for d in targets:
        pl.semaphore_signal(barrier, inc=1, device_id={"ep": d}, device_id_type=MESH)
    route()
    x_copy.wait()
    dispatch(jnp.int32(0))
    pl.semaphore_wait(barrier, n - 1)

    @pl.loop(0, local + LAG)
    def _(t):
        @pl.when(t >= LAG)
        def _():
            all_peers(*back_args(t - LAG)).wait_recv()

        @pl.when(t < local)
        def _():
            send(*fwd_args(t))
            keep_own(*fwd_args(t))

        @pl.when(t == 1)
        def _():
            gates()

            @pl.loop(0, blocks)
            def _(i):
                acc[pl.ds(pl.multiple_of(i * TILE, TILE), TILE), :] = jnp.zeros((TILE, model), jnp.float32)

        @pl.when(jnp.logical_and(t >= LAG, t < local + LAG - 1))
        def _():
            combine(t - LAG, False)

        @pl.when(jnp.logical_and(t >= 1, t <= local))
        def _():
            k = t - 1

            @pl.when(t < local)
            def _():
                for copy in weight_copies(t):
                    copy.start()

            for copy in weight_copies(k):
                copy.wait()
            all_peers(*fwd_args(k)).wait_recv()

            @pl.when(k >= 2)
            def _():
                all_peers(*back_args(k - 2)).wait_send()

            experts_ffn(k)
            send(*back_args(k))
            keep_own(*back_args(k))

        @pl.when(t + 1 < local)
        def _():
            @pl.when(t >= 1)
            def _():
                all_peers(*fwd_args(t - 1)).wait_send()

            dispatch(t + 1)

    combine(jnp.int32(local - 1), True)
    for k in range(max(local - 2, 0), local):
        all_peers(*fwd_args(jnp.int32(k))).wait_send()
        all_peers(*back_args(jnp.int32(k))).wait_send()
    pltpu.make_async_copy(x_v, out_hbm.at[0], out_sem).wait()


def solution(mesh):
    n = mesh.shape["ep"]

    def local_layer(tokens, w_gate, expert_ids, keep_second, w_in, w_out):
        _, token_count, model = tokens.shape
        experts = w_gate.shape[1]
        local, _, hidden = w_in.shape
        capacity = 2 * token_count // experts
        rows = n * capacity
        bf16, f32 = jnp.bfloat16, jnp.float32
        sizes = (token_count, model, hidden, experts, local, capacity)
        vmem, hbm = pl.BlockSpec(memory_space=pltpu.VMEM), pl.BlockSpec(memory_space=pl.ANY)
        dma = pltpu.SemaphoreType.DMA
        return pl.pallas_call(
            functools.partial(moe_kernel, n, sizes),
            out_shape=jax.ShapeDtypeStruct(tokens.shape, bf16),
            in_specs=[vmem, vmem, hbm, vmem, hbm, hbm],
            out_specs=hbm,
            scratch_shapes=[
                pltpu.VMEM((token_count, model), bf16),
                pltpu.VMEM((token_count, model), f32),
                pltpu.VMEM((2, model, hidden), bf16),
                pltpu.VMEM((2, hidden, model), bf16),
                pltpu.VMEM((2, rows, model), bf16),
                pltpu.VMEM((LAG, rows, model), bf16),
                pltpu.VMEM((2, rows, model), bf16),
                pltpu.VMEM((LAG + 1, rows, model), bf16),
                pltpu.VMEM((rows, token_count), bf16),
                pltpu.VMEM((rows, hidden), bf16),
                pltpu.VMEM((8, token_count), f32),
                pltpu.VMEM((4, token_count, 128), f32),
                dma,
                dma((2,)),
                dma((2,)),
                dma((2,)),
                dma((LAG,)),
                dma((2,)),
                dma((LAG + 1,)),
                dma,
            ],
            compiler_params=pltpu.CompilerParams(
                collective_id=0, has_side_effects=True, vmem_limit_bytes=63 * 1024 * 1024
            ),
        )(expert_ids[0].T, keep_second, tokens, w_gate, w_in, w_out)

    group_spec = P(("dp", "ep"))
    return jax.shard_map(
        local_layer,
        mesh=mesh,
        in_specs=(group_spec, P(), group_spec, group_spec, P("ep"), P("ep")),
        out_specs=group_spec,
        check_vma=False,
    )
```

```python
import functools

import jax
import jax.numpy as jnp
from jax import lax
from jax.experimental import pallas as pl
from jax.experimental.pallas import tpu as pltpu
from jax.sharding import PartitionSpec as P

MESH = pl.DeviceIdType.MESH
LAG = 3
TILE = 256
VMEM_A = 36 * 1024 * 1024
VMEM_B = 12 * 1024 * 1024


def ring_offsets(chip_count):
    near = sorted(range(1, chip_count), key=lambda d: min(d, chip_count - d))
    return near


def mix_weights(colb, base, rows, toks):
    base = jnp.int32(base).astype(jnp.float32)
    c1, c2 = colb[0, toks, :] - base, colb[1, toks, :] - base
    w1, w2 = colb[2, toks, :], colb[3, toks, :]
    parts = []
    for lane in range(0, rows, 128):
        want = (lax.broadcasted_iota(jnp.int32, (TILE, 128), 1) + lane).astype(jnp.float32)
        parts.append((jnp.where(c1 == want, w1, 0.0) + jnp.where(c2 == want, w2, 0.0)).astype(jnp.bfloat16))
    return jnp.concatenate(parts, axis=1)


def last_kernel(base, acc, colb, yrecv, out_hbm, stage, sem):
    tokens, model = acc.shape
    yslots, rows, _ = yrecv.shape
    slot = (base // rows) % yslots

    def out_copy(i):
        toks = pl.ds(pl.multiple_of(i * TILE, TILE), TILE)
        return pltpu.make_async_copy(stage.at[toks], out_hbm.at[0, toks], sem)

    @pl.loop(0, tokens // TILE)
    def _(i):
        toks = pl.ds(pl.multiple_of(i * TILE, TILE), TILE)
        mix = mix_weights(colb, base, rows, toks)
        for j in range(0, model, 2 * TILE):
            cols = pl.ds(j, 2 * TILE)
            got = acc[toks, cols] + jnp.dot(mix, yrecv[slot, :, cols], preferred_element_type=jnp.float32)
            stage[toks, cols] = got.astype(jnp.bfloat16)
        out_copy(i).start()

    pltpu.make_async_copy(stage, out_hbm.at[0], sem).wait()


def moe_kernel(
    n, sizes, ids_ref, keep_ref, x_hbm, wg_hbm, win_hbm, wout_hbm,
    acc, colb, yrecv,
    x_v, wg_v, win_v, wout_v, fsend, frecv, ysend, dmat, hid, crow,
    x_sem, wg_sem, win_sem, wout_sem, fs_sem, fr_sem, ys_sem, yr_sem,
):
    tokens, model, hidden, experts, local, capacity = sizes
    rows = n * capacity
    fslots, yslots = frecv.shape[0], yrecv.shape[0]
    shift = (local - 1).bit_length()
    blocks = tokens // TILE
    me = lax.axis_index("ep")

    def x_copy(j):
        cols = pl.ds(pl.multiple_of(j * TILE, TILE), TILE)
        return pltpu.make_async_copy(x_hbm.at[0, :, cols], x_v.at[:, cols], x_sem.at[j])

    wg_copy = pltpu.make_async_copy(wg_hbm, wg_v, wg_sem)

    def weight_copies(k):
        b = lax.rem(k, 2)
        return (
            pltpu.make_async_copy(win_hbm.at[k], win_v.at[b], win_sem.at[b]),
            pltpu.make_async_copy(wout_hbm.at[k], wout_v.at[b], wout_sem.at[b]),
        )

    def owner_rows(d):
        return pl.ds(pl.multiple_of(d * capacity, capacity), capacity)

    cores = 2 if n % 2 == 0 else 1
    chips = n // cores
    my_chip, my_core = me // cores, lax.rem(me, cores)
    targets = []
    for dist in ring_offsets(chips) + [0]:
        for c in range(cores):
            if dist == 0 and c == 0:
                continue
            targets.append(lax.rem(my_chip + dist, chips) * cores + lax.rem(my_core + c, cores))

    def send(src, src_slot, dst, dst_slot, s_sem, r_sem):
        for d in targets:
            pltpu.make_async_remote_copy(
                src_ref=src.at[src_slot, owner_rows(d)],
                dst_ref=dst.at[dst_slot, owner_rows(me)],
                send_sem=s_sem.at[src_slot],
                recv_sem=r_sem.at[dst_slot],
                device_id={"ep": d},
                device_id_type=MESH,
            ).start()

    def all_peers(src, src_slot, dst, dst_slot, s_sem, r_sem):
        part = pl.ds(0, (n - 1) * capacity)
        return pltpu.make_async_remote_copy(
            src_ref=src.at[src_slot, part],
            dst_ref=dst.at[dst_slot, part],
            send_sem=s_sem.at[src_slot],
            recv_sem=r_sem.at[dst_slot],
            device_id={"ep": me},
            device_id_type=MESH,
        )

    def fwd_args(k):
        return (fsend, lax.rem(k, 2), frecv, lax.rem(k, fslots), fs_sem, fr_sem)

    def back_args(k):
        return (ysend, lax.rem(k, 2), yrecv, lax.rem(k, yslots), ys_sem, yr_sem)

    def keep_own(src, src_slot, dst, dst_slot, *_):
        dst[dst_slot, owner_rows(me), :] = src[src_slot, owner_rows(me), :]

    def hot(blk, expert_row):
        return lax.broadcasted_iota(jnp.int32, (experts, TILE), 0) == expert_row

    def load_ids(b):
        cols = pl.ds(b * TILE, TILE)
        return ids_ref[0:1, cols], ids_ref[1:2, cols], keep_ref[0:1, cols] == 1

    def route():
        count = jnp.zeros((experts, TILE), jnp.float32)
        for b in range(blocks):
            i1, _, _ = load_ids(b)
            count = count + hot(b, i1).astype(jnp.float32)
        base1 = jnp.zeros((experts, 1), jnp.float32)
        base2 = jnp.sum(count, axis=1, keepdims=True)
        before = (
            lax.broadcasted_iota(jnp.int32, (TILE, TILE), 0) < lax.broadcasted_iota(jnp.int32, (TILE, TILE), 1)
        ).astype(jnp.bfloat16)
        for b in range(blocks):
            i1, i2, k2 = load_ids(b)
            hot1 = hot(b, i1).astype(jnp.float32)
            hot2 = jnp.where(k2, hot(b, i2).astype(jnp.float32), 0.0)
            ahead1 = jnp.dot(hot1.astype(jnp.bfloat16), before, preferred_element_type=jnp.float32) + base1
            ahead2 = jnp.dot(hot2.astype(jnp.bfloat16), before, preferred_element_type=jnp.float32) + base2
            base1 = base1 + jnp.sum(hot1, axis=1, keepdims=True)
            base2 = base2 + jnp.sum(hot2, axis=1, keepdims=True)
            pos1 = jnp.sum(ahead1 * hot1, axis=0, keepdims=True)
            pos2 = jnp.sum(ahead2 * hot2, axis=0, keepdims=True)

            def code(e, pos, kept):
                home = (e & (local - 1)) * rows + (e >> shift) * capacity
                return jnp.where(kept, home.astype(jnp.float32) + pos, -1.0)

            cols = pl.ds(b * TILE, TILE)
            crow[0:1, cols] = code(i1, pos1, pos1 < capacity)
            crow[1:2, cols] = code(i2, pos2, jnp.logical_and(k2, pos2 < capacity))

    def gates():
        for b in range(blocks):
            cols = pl.ds(b * TILE, TILE)
            i1, i2, k2 = load_ids(b)
            logits = jnp.dot(x_v[cols, :], wg_v[...], preferred_element_type=jnp.float32).T
            top = jnp.max(logits, axis=0, keepdims=True)
            grown = jnp.exp(logits - top)
            probs = grown / jnp.sum(grown, axis=0, keepdims=True)
            g1 = jnp.sum(jnp.where(hot(b, i1), probs, 0.0), axis=0, keepdims=True)
            g2 = jnp.where(k2, jnp.sum(jnp.where(hot(b, i2), probs, 0.0), axis=0, keepdims=True), 0.0)
            total = g1 + g2
            for q, row in enumerate((crow[0:1, cols], crow[1:2, cols], g1 / total, g2 / total)):
                colb[q, cols, :] = jnp.broadcast_to(row, (128, TILE)).T

    def dispatch(k, first=False):
        slot = lax.rem(k, 2)
        base = (k * rows).astype(jnp.float32)
        for b in range(blocks):
            cols = pl.ds(b * TILE, TILE)
            want = lax.broadcasted_iota(jnp.int32, (rows, TILE), 0).astype(jnp.float32)
            c1, c2 = crow[0:1, cols] - base, crow[1:2, cols] - base
            dmat[:, cols] = jnp.where(jnp.logical_or(c1 == want, c2 == want), 1.0, 0.0).astype(jnp.bfloat16)

        @pl.loop(0, model // TILE)
        def _(j):
            if first:
                x_copy(j).wait()
            cols = pl.ds(pl.multiple_of(j * TILE, TILE), TILE)
            fsend[slot, :, cols] = jnp.dot(
                dmat[...], x_v[:, cols], preferred_element_type=jnp.float32
            ).astype(jnp.bfloat16)

    def experts_ffn(k):
        w, slot, out_slot = lax.rem(k, 2), lax.rem(k, fslots), lax.rem(k, 2)

        @pl.loop(0, hidden // TILE)
        def _(j):
            cols = pl.ds(pl.multiple_of(j * TILE, TILE), TILE)
            h = jnp.dot(frecv[slot], win_v[w, :, cols], preferred_element_type=jnp.float32)
            hid[:, cols] = jnp.maximum(h, 0.0).astype(jnp.bfloat16)

        @pl.loop(0, model // TILE)
        def _(j):
            cols = pl.ds(pl.multiple_of(j * TILE, TILE), TILE)
            y = jnp.dot(hid[...], wout_v[w, :, cols], preferred_element_type=jnp.float32)
            ysend[out_slot, :, cols] = y.astype(jnp.bfloat16)

    def combine(k):
        @pl.loop(0, blocks)
        def _(i):
            toks = pl.ds(pl.multiple_of(i * TILE, TILE), TILE)
            mix = mix_weights(colb, k * rows, rows, toks)
            for j in range(0, model, 2 * TILE):
                cols = pl.ds(j, 2 * TILE)
                acc[toks, cols] += jnp.dot(
                    mix, yrecv[lax.rem(k, yslots), :, cols], preferred_element_type=jnp.float32
                )

    for j in range(model // TILE):
        x_copy(j).start()
    barrier = pltpu.get_barrier_semaphore()
    for d in targets:
        pl.semaphore_signal(barrier, inc=1, device_id={"ep": d}, device_id_type=MESH)
    route()
    wg_copy.start()
    for copy in weight_copies(0):
        copy.start()
    dispatch(jnp.int32(0), first=True)
    pl.semaphore_wait(barrier, n - 1)

    @pl.loop(0, local + LAG)
    def _(t):
        @pl.when(t >= LAG)
        def _():
            all_peers(*back_args(t - LAG)).wait_recv()

        @pl.when(t < local)
        def _():
            send(*fwd_args(t))
            keep_own(*fwd_args(t))

        @pl.when(t == 1)
        def _():
            wg_copy.wait()
            gates()

            @pl.loop(0, blocks)
            def _(i):
                acc[pl.ds(pl.multiple_of(i * TILE, TILE), TILE), :] = jnp.zeros((TILE, model), jnp.float32)

        @pl.when(jnp.logical_and(t >= LAG, t < local + LAG - 1))
        def _():
            combine(t - LAG)

        @pl.when(jnp.logical_and(t >= 1, t <= local))
        def _():
            k = t - 1

            @pl.when(t < local)
            def _():
                for copy in weight_copies(t):
                    copy.start()

            for copy in weight_copies(k):
                copy.wait()
            all_peers(*fwd_args(k)).wait_recv()

            @pl.when(k >= 2)
            def _():
                all_peers(*back_args(k - 2)).wait_send()

            experts_ffn(k)
            send(*back_args(k))
            keep_own(*back_args(k))

        @pl.when(t + 1 < local)
        def _():
            @pl.when(t >= 1)
            def _():
                all_peers(*fwd_args(t - 1)).wait_send()

            dispatch(t + 1)

    for k in range(max(local - 2, 0), local):
        all_peers(*fwd_args(jnp.int32(k))).wait_send()
        all_peers(*back_args(jnp.int32(k))).wait_send()


def solution(mesh):
    n = mesh.shape["ep"]

    def local_layer(tokens, w_gate, expert_ids, keep_second, w_in, w_out):
        _, token_count, model = tokens.shape
        experts = w_gate.shape[1]
        local, _, hidden = w_in.shape
        capacity = 2 * token_count // experts
        rows = n * capacity
        bf16, f32 = jnp.bfloat16, jnp.float32
        sizes = (token_count, model, hidden, experts, local, capacity)
        vmem, hbm = pl.BlockSpec(memory_space=pltpu.VMEM), pl.BlockSpec(memory_space=pl.ANY)
        dma = pltpu.SemaphoreType.DMA
        acc, colb, yrecv = pl.pallas_call(
            functools.partial(moe_kernel, n, sizes),
            out_shape=(
                pltpu.VMEM((token_count, model), f32),
                pltpu.VMEM((4, token_count, 128), f32),
                pltpu.VMEM((LAG + 1, rows, model), bf16),
            ),
            in_specs=[vmem, vmem, hbm, hbm, hbm, hbm],
            out_specs=(vmem, vmem, vmem),
            scratch_shapes=[
                pltpu.VMEM((token_count, model), bf16),
                pltpu.VMEM(w_gate.shape, bf16),
                pltpu.VMEM((2, model, hidden), bf16),
                pltpu.VMEM((2, hidden, model), bf16),
                pltpu.VMEM((2, rows, model), bf16),
                pltpu.VMEM((LAG, rows, model), bf16),
                pltpu.VMEM((2, rows, model), bf16),
                pltpu.VMEM((rows, token_count), bf16),
                pltpu.VMEM((rows, hidden), bf16),
                pltpu.VMEM((8, token_count), f32),
                dma((model // TILE,)),
                dma,
                dma((2,)),
                dma((2,)),
                dma((2,)),
                dma((LAG,)),
                dma((2,)),
                dma((LAG + 1,)),
            ],
            compiler_params=pltpu.CompilerParams(
                collective_id=0, has_side_effects=True, vmem_limit_bytes=VMEM_A
            ),
        )(expert_ids[0].T, keep_second, tokens, w_gate, w_in, w_out)
        return pl.pallas_call(
            functools.partial(last_kernel, (local - 1) * rows),
            out_shape=jax.ShapeDtypeStruct(tokens.shape, bf16),
            in_specs=[vmem, vmem, vmem],
            out_specs=hbm,
            scratch_shapes=[pltpu.VMEM((token_count, model), bf16), dma],
            compiler_params=pltpu.CompilerParams(vmem_limit_bytes=VMEM_B),
        )(acc, colb, yrecv)

    group_spec = P(("dp", "ep"))
    return jax.shard_map(
        local_layer,
        mesh=mesh,
        in_specs=(group_spec, P(), group_spec, group_spec, P("ep"), P("ep")),
        out_specs=group_spec,
        check_vma=False,
    )
```

```python
import functools

import jax
import jax.numpy as jnp
from jax import lax
from jax.experimental import pallas as pl
from jax.experimental.pallas import tpu as pltpu
from jax.sharding import PartitionSpec as P

MESH = pl.DeviceIdType.MESH
LAG = 3
TILE = 256
PIECE = 512
VMEM_A = 36 * 1024 * 1024
VMEM_B = 12 * 1024 * 1024


def ring_offsets(chip_count):
    near = sorted(range(1, chip_count), key=lambda d: min(d, chip_count - d))
    return near


def mix_weights(colb, base, rows, toks):
    base = jnp.int32(base).astype(jnp.float32)
    c1, c2 = colb[0, toks, :] - base, colb[1, toks, :] - base
    w1, w2 = colb[2, toks, :], colb[3, toks, :]
    parts = []
    for lane in range(0, rows, 128):
        want = (lax.broadcasted_iota(jnp.int32, (TILE, 128), 1) + lane).astype(jnp.float32)
        parts.append((jnp.where(c1 == want, w1, 0.0) + jnp.where(c2 == want, w2, 0.0)).astype(jnp.bfloat16))
    return jnp.concatenate(parts, axis=1)


def last_kernel(base, acc, colb, yrecv, out_hbm, stage, sem):
    tokens, model = acc.shape
    yslots, rows, _ = yrecv.shape
    slot = (base // rows) % yslots

    def out_copy(i):
        toks = pl.ds(pl.multiple_of(i * TILE, TILE), TILE)
        return pltpu.make_async_copy(stage.at[toks], out_hbm.at[0, toks], sem)

    @pl.loop(0, tokens // TILE)
    def _(i):
        toks = pl.ds(pl.multiple_of(i * TILE, TILE), TILE)
        mix = mix_weights(colb, base, rows, toks)
        for j in range(0, model, 2 * TILE):
            cols = pl.ds(j, 2 * TILE)
            got = acc[toks, cols] + jnp.dot(mix, yrecv[slot, :, cols], preferred_element_type=jnp.float32)
            stage[toks, cols] = got.astype(jnp.bfloat16)
        out_copy(i).start()

    pltpu.make_async_copy(stage, out_hbm.at[0], sem).wait()


def moe_kernel(
    n, sizes, ids_hbm, keep_hbm, x_hbm, wg_hbm, win_hbm, wout_hbm,
    acc, colb, yrecv,
    ids_ref, keep_ref, x_v, wg_v, win_v, wout_v, fsend, frecv, ysend, dmat, hid, crow,
    id_sem, x_sem, wg_sem, win_sem, wout_sem, fs_sem, fr_sem, ys_sem, yr_sem,
):
    tokens, model, hidden, experts, local, capacity = sizes
    rows = n * capacity
    fslots, yslots = frecv.shape[0], yrecv.shape[0]
    shift = (local - 1).bit_length()
    blocks = tokens // TILE
    me = lax.axis_index("ep")

    def x_copy(j):
        cols = pl.ds(pl.multiple_of(j * TILE, TILE), TILE)
        return pltpu.make_async_copy(x_hbm.at[0, :, cols], x_v.at[:, cols], x_sem.at[j])

    id_copies = (
        pltpu.make_async_copy(ids_hbm, ids_ref, id_sem.at[0]),
        pltpu.make_async_copy(keep_hbm, keep_ref, id_sem.at[1]),
    )
    wg_copy = pltpu.make_async_copy(wg_hbm, wg_v, wg_sem)

    def weight_copies(k):
        b = lax.rem(k, 2)
        return (
            pltpu.make_async_copy(win_hbm.at[k], win_v.at[b], win_sem.at[b]),
            pltpu.make_async_copy(wout_hbm.at[k], wout_v.at[b], wout_sem.at[b]),
        )

    def owner_rows(d):
        return pl.ds(pl.multiple_of(d * capacity, capacity), capacity)

    cores = 2 if n % 2 == 0 else 1
    chips = n // cores
    my_chip, my_core = me // cores, lax.rem(me, cores)
    targets = []
    for dist in ring_offsets(chips) + [0]:
        for c in range(cores):
            if dist == 0 and c == 0:
                continue
            targets.append(lax.rem(my_chip + dist, chips) * cores + lax.rem(my_core + c, cores))

    def send(src, src_slot, dst, dst_slot, s_sem, r_sem, cols=slice(None)):
        for d in targets:
            pltpu.make_async_remote_copy(
                src_ref=src.at[src_slot, owner_rows(d), cols],
                dst_ref=dst.at[dst_slot, owner_rows(me), cols],
                send_sem=s_sem.at[src_slot],
                recv_sem=r_sem.at[dst_slot],
                device_id={"ep": d},
                device_id_type=MESH,
            ).start()

    def all_peers(src, src_slot, dst, dst_slot, s_sem, r_sem):
        part = pl.ds(0, (n - 1) * capacity)
        return pltpu.make_async_remote_copy(
            src_ref=src.at[src_slot, part],
            dst_ref=dst.at[dst_slot, part],
            send_sem=s_sem.at[src_slot],
            recv_sem=r_sem.at[dst_slot],
            device_id={"ep": me},
            device_id_type=MESH,
        )

    def fwd_args(k):
        return (fsend, lax.rem(k, 2), frecv, lax.rem(k, fslots), fs_sem, fr_sem)

    def back_args(k):
        return (ysend, lax.rem(k, 2), yrecv, lax.rem(k, yslots), ys_sem, yr_sem)

    def keep_own(src, src_slot, dst, dst_slot, *_):
        dst[dst_slot, owner_rows(me), :] = src[src_slot, owner_rows(me), :]

    def hot(blk, expert_row):
        return lax.broadcasted_iota(jnp.int32, (experts, TILE), 0) == expert_row

    def load_ids(b):
        cols = pl.ds(b * TILE, TILE)
        return ids_ref[0:1, cols], ids_ref[1:2, cols], keep_ref[0:1, cols] == 1

    def route():
        count = jnp.zeros((experts, TILE), jnp.float32)
        for b in range(blocks):
            i1, _, _ = load_ids(b)
            count = count + hot(b, i1).astype(jnp.float32)
        base1 = jnp.zeros((experts, 1), jnp.float32)
        base2 = jnp.sum(count, axis=1, keepdims=True)
        before = (
            lax.broadcasted_iota(jnp.int32, (TILE, TILE), 0) < lax.broadcasted_iota(jnp.int32, (TILE, TILE), 1)
        ).astype(jnp.bfloat16)
        for b in range(blocks):
            i1, i2, k2 = load_ids(b)
            hot1 = hot(b, i1).astype(jnp.float32)
            hot2 = jnp.where(k2, hot(b, i2).astype(jnp.float32), 0.0)
            ahead1 = jnp.dot(hot1.astype(jnp.bfloat16), before, preferred_element_type=jnp.float32) + base1
            ahead2 = jnp.dot(hot2.astype(jnp.bfloat16), before, preferred_element_type=jnp.float32) + base2
            base1 = base1 + jnp.sum(hot1, axis=1, keepdims=True)
            base2 = base2 + jnp.sum(hot2, axis=1, keepdims=True)
            pos1 = jnp.sum(ahead1 * hot1, axis=0, keepdims=True)
            pos2 = jnp.sum(ahead2 * hot2, axis=0, keepdims=True)

            def code(e, pos, kept):
                home = (e & (local - 1)) * rows + (e >> shift) * capacity
                return jnp.where(kept, home.astype(jnp.float32) + pos, -1.0)

            cols = pl.ds(b * TILE, TILE)
            crow[0:1, cols] = code(i1, pos1, pos1 < capacity)
            crow[1:2, cols] = code(i2, pos2, jnp.logical_and(k2, pos2 < capacity))

    def gates():
        for b in range(blocks):
            cols = pl.ds(b * TILE, TILE)
            i1, i2, k2 = load_ids(b)
            logits = jnp.dot(x_v[cols, :], wg_v[...], preferred_element_type=jnp.float32).T
            top = jnp.max(logits, axis=0, keepdims=True)
            grown = jnp.exp(logits - top)
            probs = grown / jnp.sum(grown, axis=0, keepdims=True)
            g1 = jnp.sum(jnp.where(hot(b, i1), probs, 0.0), axis=0, keepdims=True)
            g2 = jnp.where(k2, jnp.sum(jnp.where(hot(b, i2), probs, 0.0), axis=0, keepdims=True), 0.0)
            total = g1 + g2
            for q, row in enumerate((crow[0:1, cols], crow[1:2, cols], g1 / total, g2 / total)):
                colb[q, cols, :] = jnp.broadcast_to(row, (128, TILE)).T

    def dispatch_mask(k):
        base = (k * rows).astype(jnp.float32)
        for b in range(blocks):
            cols = pl.ds(b * TILE, TILE)
            want = lax.broadcasted_iota(jnp.int32, (rows, TILE), 0).astype(jnp.float32)
            c1, c2 = crow[0:1, cols] - base, crow[1:2, cols] - base
            dmat[:, cols] = jnp.where(jnp.logical_or(c1 == want, c2 == want), 1.0, 0.0).astype(jnp.bfloat16)

    def dispatch_tile(slot, j):
        cols = pl.ds(pl.multiple_of(j * TILE, TILE), TILE)
        fsend[slot, :, cols] = jnp.dot(dmat[...], x_v[:, cols], preferred_element_type=jnp.float32).astype(jnp.bfloat16)

    def dispatch(k):
        dispatch_mask(k)

        @pl.loop(0, model // TILE)
        def _(j):
            dispatch_tile(lax.rem(k, 2), j)

    def experts_ffn(k):
        w, slot, out_slot = lax.rem(k, 2), lax.rem(k, fslots), lax.rem(k, 2)

        @pl.loop(0, hidden // TILE)
        def _(j):
            cols = pl.ds(pl.multiple_of(j * TILE, TILE), TILE)
            h = jnp.dot(frecv[slot], win_v[w, :, cols], preferred_element_type=jnp.float32)
            hid[:, cols] = jnp.maximum(h, 0.0).astype(jnp.bfloat16)

        @pl.loop(0, model // TILE)
        def _(j):
            cols = pl.ds(pl.multiple_of(j * TILE, TILE), TILE)
            y = jnp.dot(hid[...], wout_v[w, :, cols], preferred_element_type=jnp.float32)
            ysend[out_slot, :, cols] = y.astype(jnp.bfloat16)

    def combine(k):
        @pl.loop(0, blocks)
        def _(i):
            toks = pl.ds(pl.multiple_of(i * TILE, TILE), TILE)
            mix = mix_weights(colb, k * rows, rows, toks)
            for j in range(0, model, 2 * TILE):
                cols = pl.ds(j, 2 * TILE)
                acc[toks, cols] += jnp.dot(
                    mix, yrecv[lax.rem(k, yslots), :, cols], preferred_element_type=jnp.float32
                )

    for copy in id_copies:
        copy.start()
    for j in range(model // TILE):
        x_copy(j).start()
    barrier = pltpu.get_barrier_semaphore()
    for d in targets:
        pl.semaphore_signal(barrier, inc=1, device_id={"ep": d}, device_id_type=MESH)
    for copy in id_copies:
        copy.wait()
    route()
    wg_copy.start()
    for copy in weight_copies(0):
        copy.start()
    first = jnp.int32(0)
    dispatch_mask(first)
    pl.semaphore_wait(barrier, n - 1)

    @pl.loop(0, model // PIECE)
    def _(piece):
        for j in range(PIECE // TILE):
            x_copy(piece * (PIECE // TILE) + j).wait()
            dispatch_tile(0, piece * (PIECE // TILE) + j)
        send(*fwd_args(first), pl.ds(pl.multiple_of(piece * PIECE, PIECE), PIECE))

    keep_own(*fwd_args(first))

    @pl.loop(0, local + LAG)
    def _(t):
        @pl.when(t >= LAG)
        def _():
            all_peers(*back_args(t - LAG)).wait_recv()

        @pl.when(jnp.logical_and(t >= 1, t < local))
        def _():
            send(*fwd_args(t))
            keep_own(*fwd_args(t))

        @pl.when(t == 1)
        def _():
            wg_copy.wait()
            gates()

            @pl.loop(0, blocks)
            def _(i):
                acc[pl.ds(pl.multiple_of(i * TILE, TILE), TILE), :] = jnp.zeros((TILE, model), jnp.float32)

        @pl.when(jnp.logical_and(t >= LAG, t < local + LAG - 1))
        def _():
            combine(t - LAG)

        @pl.when(jnp.logical_and(t >= 1, t <= local))
        def _():
            k = t - 1

            @pl.when(t < local)
            def _():
                for copy in weight_copies(t):
                    copy.start()

            for copy in weight_copies(k):
                copy.wait()
            all_peers(*fwd_args(k)).wait_recv()

            @pl.when(k >= 2)
            def _():
                all_peers(*back_args(k - 2)).wait_send()

            experts_ffn(k)
            send(*back_args(k))
            keep_own(*back_args(k))

        @pl.when(t + 1 < local)
        def _():
            @pl.when(t >= 1)
            def _():
                all_peers(*fwd_args(t - 1)).wait_send()

            dispatch(t + 1)

    for k in range(max(local - 2, 0), local):
        all_peers(*fwd_args(jnp.int32(k))).wait_send()
        all_peers(*back_args(jnp.int32(k))).wait_send()


def solution(mesh):
    n = mesh.shape["ep"]

    def local_layer(tokens, w_gate, expert_ids, keep_second, w_in, w_out):
        _, token_count, model = tokens.shape
        experts = w_gate.shape[1]
        local, _, hidden = w_in.shape
        capacity = 2 * token_count // experts
        rows = n * capacity
        bf16, f32 = jnp.bfloat16, jnp.float32
        sizes = (token_count, model, hidden, experts, local, capacity)
        vmem, hbm = pl.BlockSpec(memory_space=pltpu.VMEM), pl.BlockSpec(memory_space=pl.ANY)
        dma = pltpu.SemaphoreType.DMA
        acc, colb, yrecv = pl.pallas_call(
            functools.partial(moe_kernel, n, sizes),
            out_shape=(
                pltpu.VMEM((token_count, model), f32),
                pltpu.VMEM((4, token_count, 128), f32),
                pltpu.VMEM((LAG + 1, rows, model), bf16),
            ),
            in_specs=[hbm] * 6,
            out_specs=(vmem, vmem, vmem),
            scratch_shapes=[
                pltpu.VMEM((2, token_count), jnp.int32),
                pltpu.VMEM((1, token_count), jnp.int32),
                pltpu.VMEM((token_count, model), bf16),
                pltpu.VMEM(w_gate.shape, bf16),
                pltpu.VMEM((2, model, hidden), bf16),
                pltpu.VMEM((2, hidden, model), bf16),
                pltpu.VMEM((2, rows, model), bf16),
                pltpu.VMEM((LAG, rows, model), bf16),
                pltpu.VMEM((2, rows, model), bf16),
                pltpu.VMEM((rows, token_count), bf16),
                pltpu.VMEM((rows, hidden), bf16),
                pltpu.VMEM((8, token_count), f32),
                dma((2,)),
                dma((model // TILE,)),
                dma,
                dma((2,)),
                dma((2,)),
                dma((2,)),
                dma((LAG,)),
                dma((2,)),
                dma((LAG + 1,)),
            ],
            compiler_params=pltpu.CompilerParams(
                collective_id=0, has_side_effects=True, vmem_limit_bytes=VMEM_A
            ),
        )(expert_ids[0].T, keep_second, tokens, w_gate, w_in, w_out)
        return pl.pallas_call(
            functools.partial(last_kernel, (local - 1) * rows),
            out_shape=jax.ShapeDtypeStruct(tokens.shape, bf16),
            in_specs=[vmem, vmem, vmem],
            out_specs=hbm,
            scratch_shapes=[pltpu.VMEM((token_count, model), bf16), dma],
            compiler_params=pltpu.CompilerParams(vmem_limit_bytes=VMEM_B),
        )(acc, colb, yrecv)

    group_spec = P(("dp", "ep"))
    return jax.shard_map(
        local_layer,
        mesh=mesh,
        in_specs=(group_spec, P(), group_spec, group_spec, P("ep"), P("ep")),
        out_specs=group_spec,
        check_vma=False,
    )
```

```python
import functools

import jax
import jax.numpy as jnp
from jax import lax
from jax.experimental import pallas as pl
from jax.experimental.pallas import tpu as pltpu
from jax.sharding import PartitionSpec as P

MESH = pl.DeviceIdType.MESH
FFN_LAG = 2
LAG = 4
RESULTS = 3
TILE = 256
PIECE = 512
VMEM_A = 36 * 1024 * 1024
VMEM_B = 12 * 1024 * 1024


def ring_offsets(chip_count):
    near = sorted(range(1, chip_count), key=lambda d: min(d, chip_count - d))
    return near


def mix_weights(colb, base, rows, toks):
    base = jnp.int32(base).astype(jnp.float32)
    c1, c2 = colb[0, toks, :] - base, colb[1, toks, :] - base
    w1, w2 = colb[2, toks, :], colb[3, toks, :]
    parts = []
    for lane in range(0, rows, 128):
        want = (lax.broadcasted_iota(jnp.int32, (TILE, 128), 1) + lane).astype(jnp.float32)
        parts.append((jnp.where(c1 == want, w1, 0.0) + jnp.where(c2 == want, w2, 0.0)).astype(jnp.bfloat16))
    return jnp.concatenate(parts, axis=1)


def last_kernel(base, acc, colb, yrecv, out_hbm, stage, sem):
    tokens, model = acc.shape
    yslots, rows, _ = yrecv.shape
    slot = (base // rows) % yslots

    def out_copy(i):
        toks = pl.ds(pl.multiple_of(i * TILE, TILE), TILE)
        return pltpu.make_async_copy(stage.at[toks], out_hbm.at[0, toks], sem)

    @pl.loop(0, tokens // TILE)
    def _(i):
        toks = pl.ds(pl.multiple_of(i * TILE, TILE), TILE)
        mix = mix_weights(colb, base, rows, toks)
        for j in range(0, model, 2 * TILE):
            cols = pl.ds(j, 2 * TILE)
            got = acc[toks, cols] + jnp.dot(mix, yrecv[slot, :, cols], preferred_element_type=jnp.float32)
            stage[toks, cols] = got.astype(jnp.bfloat16)
        out_copy(i).start()

    pltpu.make_async_copy(stage, out_hbm.at[0], sem).wait()


def moe_kernel(
    n, sizes, ids_hbm, keep_hbm, x_hbm, wg_hbm, win_hbm, wout_hbm,
    acc, colb, yrecv,
    ids_ref, keep_ref, x_v, wg_v, win_v, wout_v, fsend, frecv, ysend, dmat, hid, crow,
    id_sem, x_sem, wg_sem, win_sem, wout_sem, fs_sem, fr_sem, ys_sem, yr_sem,
):
    tokens, model, hidden, experts, local, capacity = sizes
    rows = n * capacity
    fslots, yslots = frecv.shape[0], yrecv.shape[0]
    shift = (local - 1).bit_length()
    blocks = tokens // TILE
    me = lax.axis_index("ep")

    def x_copy(j):
        cols = pl.ds(pl.multiple_of(j * TILE, TILE), TILE)
        return pltpu.make_async_copy(x_hbm.at[0, :, cols], x_v.at[:, cols], x_sem.at[j])

    id_copies = (
        pltpu.make_async_copy(ids_hbm, ids_ref, id_sem.at[0]),
        pltpu.make_async_copy(keep_hbm, keep_ref, id_sem.at[1]),
    )
    wg_copy = pltpu.make_async_copy(wg_hbm, wg_v, wg_sem)

    def weight_copies(k):
        b = lax.rem(k, 2)
        return (
            pltpu.make_async_copy(win_hbm.at[k], win_v.at[b], win_sem.at[b]),
            pltpu.make_async_copy(wout_hbm.at[k], wout_v.at[b], wout_sem.at[b]),
        )

    def owner_rows(d):
        return pl.ds(pl.multiple_of(d * capacity, capacity), capacity)

    cores = 2 if n % 2 == 0 else 1
    chips = n // cores
    my_chip, my_core = me // cores, lax.rem(me, cores)
    targets = []
    for dist in ring_offsets(chips) + [0]:
        for c in range(cores):
            if dist == 0 and c == 0:
                continue
            targets.append(lax.rem(my_chip + dist, chips) * cores + lax.rem(my_core + c, cores))

    def send(src, src_slot, dst, dst_slot, s_sem, r_sem, cols=slice(None)):
        for d in targets:
            pltpu.make_async_remote_copy(
                src_ref=src.at[src_slot, owner_rows(d), cols],
                dst_ref=dst.at[dst_slot, owner_rows(me), cols],
                send_sem=s_sem.at[src_slot],
                recv_sem=r_sem.at[dst_slot],
                device_id={"ep": d},
                device_id_type=MESH,
            ).start()

    def all_peers(src, src_slot, dst, dst_slot, s_sem, r_sem):
        part = pl.ds(0, (n - 1) * capacity)
        return pltpu.make_async_remote_copy(
            src_ref=src.at[src_slot, part],
            dst_ref=dst.at[dst_slot, part],
            send_sem=s_sem.at[src_slot],
            recv_sem=r_sem.at[dst_slot],
            device_id={"ep": me},
            device_id_type=MESH,
        )

    def fwd_args(k):
        return (fsend, lax.rem(k, 2), frecv, lax.rem(k, fslots), fs_sem, fr_sem)

    def back_args(k):
        return (ysend, lax.rem(k, RESULTS), yrecv, lax.rem(k, yslots), ys_sem, yr_sem)

    def keep_own(src, src_slot, dst, dst_slot, *_):
        dst[dst_slot, owner_rows(me), :] = src[src_slot, owner_rows(me), :]

    def hot(blk, expert_row):
        return lax.broadcasted_iota(jnp.int32, (experts, TILE), 0) == expert_row

    def load_ids(b):
        cols = pl.ds(b * TILE, TILE)
        return ids_ref[0:1, cols], ids_ref[1:2, cols], keep_ref[0:1, cols] == 1

    def route():
        count = jnp.zeros((experts, TILE), jnp.float32)
        for b in range(blocks):
            i1, _, _ = load_ids(b)
            count = count + hot(b, i1).astype(jnp.float32)
        base1 = jnp.zeros((experts, 1), jnp.float32)
        base2 = jnp.sum(count, axis=1, keepdims=True)
        before = (
            lax.broadcasted_iota(jnp.int32, (TILE, TILE), 0) < lax.broadcasted_iota(jnp.int32, (TILE, TILE), 1)
        ).astype(jnp.bfloat16)
        for b in range(blocks):
            i1, i2, k2 = load_ids(b)
            hot1 = hot(b, i1).astype(jnp.float32)
            hot2 = jnp.where(k2, hot(b, i2).astype(jnp.float32), 0.0)
            ahead1 = jnp.dot(hot1.astype(jnp.bfloat16), before, preferred_element_type=jnp.float32) + base1
            ahead2 = jnp.dot(hot2.astype(jnp.bfloat16), before, preferred_element_type=jnp.float32) + base2
            base1 = base1 + jnp.sum(hot1, axis=1, keepdims=True)
            base2 = base2 + jnp.sum(hot2, axis=1, keepdims=True)
            pos1 = jnp.sum(ahead1 * hot1, axis=0, keepdims=True)
            pos2 = jnp.sum(ahead2 * hot2, axis=0, keepdims=True)

            def code(e, pos, kept):
                home = (e & (local - 1)) * rows + (e >> shift) * capacity
                return jnp.where(kept, home.astype(jnp.float32) + pos, -1.0)

            cols = pl.ds(b * TILE, TILE)
            crow[0:1, cols] = code(i1, pos1, pos1 < capacity)
            crow[1:2, cols] = code(i2, pos2, jnp.logical_and(k2, pos2 < capacity))

    def gates():
        for b in range(blocks):
            cols = pl.ds(b * TILE, TILE)
            i1, i2, k2 = load_ids(b)
            logits = jnp.dot(x_v[cols, :], wg_v[...], preferred_element_type=jnp.float32).T
            top = jnp.max(logits, axis=0, keepdims=True)
            grown = jnp.exp(logits - top)
            probs = grown / jnp.sum(grown, axis=0, keepdims=True)
            g1 = jnp.sum(jnp.where(hot(b, i1), probs, 0.0), axis=0, keepdims=True)
            g2 = jnp.where(k2, jnp.sum(jnp.where(hot(b, i2), probs, 0.0), axis=0, keepdims=True), 0.0)
            total = g1 + g2
            for q, row in enumerate((crow[0:1, cols], crow[1:2, cols], g1 / total, g2 / total)):
                colb[q, cols, :] = jnp.broadcast_to(row, (128, TILE)).T

    def dispatch_mask(k):
        base = (k * rows).astype(jnp.float32)
        for b in range(blocks):
            cols = pl.ds(b * TILE, TILE)
            want = lax.broadcasted_iota(jnp.int32, (rows, TILE), 0).astype(jnp.float32)
            c1, c2 = crow[0:1, cols] - base, crow[1:2, cols] - base
            dmat[:, cols] = jnp.where(jnp.logical_or(c1 == want, c2 == want), 1.0, 0.0).astype(jnp.bfloat16)

    def dispatch_tile(slot, j):
        cols = pl.ds(pl.multiple_of(j * TILE, TILE), TILE)
        fsend[slot, :, cols] = jnp.dot(dmat[...], x_v[:, cols], preferred_element_type=jnp.float32).astype(jnp.bfloat16)

    def dispatch(k):
        dispatch_mask(k)

        @pl.loop(0, model // TILE)
        def _(j):
            dispatch_tile(lax.rem(k, 2), j)

    def experts_ffn(k):
        w, slot, out_slot = lax.rem(k, 2), lax.rem(k, fslots), lax.rem(k, RESULTS)

        @pl.loop(0, hidden // TILE)
        def _(j):
            cols = pl.ds(pl.multiple_of(j * TILE, TILE), TILE)
            h = jnp.dot(frecv[slot], win_v[w, :, cols], preferred_element_type=jnp.float32)
            hid[:, cols] = jnp.maximum(h, 0.0).astype(jnp.bfloat16)

        @pl.loop(0, model // TILE)
        def _(j):
            cols = pl.ds(pl.multiple_of(j * TILE, TILE), TILE)
            y = jnp.dot(hid[...], wout_v[w, :, cols], preferred_element_type=jnp.float32)
            ysend[out_slot, :, cols] = y.astype(jnp.bfloat16)

    def combine(k):
        @pl.loop(0, blocks)
        def _(i):
            toks = pl.ds(pl.multiple_of(i * TILE, TILE), TILE)
            mix = mix_weights(colb, k * rows, rows, toks)
            for j in range(0, model, 2 * TILE):
                cols = pl.ds(j, 2 * TILE)
                acc[toks, cols] += jnp.dot(
                    mix, yrecv[lax.rem(k, yslots), :, cols], preferred_element_type=jnp.float32
                )

    for copy in id_copies:
        copy.start()
    for j in range(model // TILE):
        x_copy(j).start()
    barrier = pltpu.get_barrier_semaphore()
    for d in targets:
        pl.semaphore_signal(barrier, inc=1, device_id={"ep": d}, device_id_type=MESH)
    for copy in id_copies:
        copy.wait()
    route()
    wg_copy.start()
    for copy in weight_copies(0):
        copy.start()
    first = jnp.int32(0)
    dispatch_mask(first)
    pl.semaphore_wait(barrier, n - 1)

    @pl.loop(0, model // PIECE)
    def _(piece):
        for j in range(PIECE // TILE):
            x_copy(piece * (PIECE // TILE) + j).wait()
            dispatch_tile(0, piece * (PIECE // TILE) + j)
        send(*fwd_args(first), pl.ds(pl.multiple_of(piece * PIECE, PIECE), PIECE))

    keep_own(*fwd_args(first))

    @pl.loop(0, local + LAG)
    def _(t):
        @pl.when(t >= LAG)
        def _():
            all_peers(*back_args(t - LAG)).wait_recv()

        @pl.when(jnp.logical_and(t >= 1, t < local))
        def _():
            send(*fwd_args(t))
            keep_own(*fwd_args(t))

        @pl.when(t == 1)
        def _():
            wg_copy.wait()
            gates()

            @pl.loop(0, blocks)
            def _(i):
                acc[pl.ds(pl.multiple_of(i * TILE, TILE), TILE), :] = jnp.zeros((TILE, model), jnp.float32)

        @pl.when(jnp.logical_and(t >= LAG, t < local + LAG - 1))
        def _():
            combine(t - LAG)

        @pl.when(jnp.logical_and(t >= FFN_LAG, t < local + FFN_LAG))
        def _():
            k = t - FFN_LAG

            @pl.when(k + 1 < local)
            def _():
                for copy in weight_copies(k + 1):
                    copy.start()

            for copy in weight_copies(k):
                copy.wait()
            all_peers(*fwd_args(k)).wait_recv()

            @pl.when(k >= RESULTS)
            def _():
                all_peers(*back_args(k - RESULTS)).wait_send()

            experts_ffn(k)
            send(*back_args(k))
            keep_own(*back_args(k))

        @pl.when(t + 1 < local)
        def _():
            @pl.when(t >= 1)
            def _():
                all_peers(*fwd_args(t - 1)).wait_send()

            dispatch(t + 1)

    for k in range(max(local - 2, 0), local):
        all_peers(*fwd_args(jnp.int32(k))).wait_send()
    for k in range(max(local - RESULTS, 0), local):
        all_peers(*back_args(jnp.int32(k))).wait_send()


def solution(mesh):
    n = mesh.shape["ep"]

    def local_layer(tokens, w_gate, expert_ids, keep_second, w_in, w_out):
        _, token_count, model = tokens.shape
        experts = w_gate.shape[1]
        local, _, hidden = w_in.shape
        capacity = 2 * token_count // experts
        rows = n * capacity
        bf16, f32 = jnp.bfloat16, jnp.float32
        sizes = (token_count, model, hidden, experts, local, capacity)
        vmem, hbm = pl.BlockSpec(memory_space=pltpu.VMEM), pl.BlockSpec(memory_space=pl.ANY)
        dma = pltpu.SemaphoreType.DMA
        acc, colb, yrecv = pl.pallas_call(
            functools.partial(moe_kernel, n, sizes),
            out_shape=(
                pltpu.VMEM((token_count, model), f32),
                pltpu.VMEM((4, token_count, 128), f32),
                pltpu.VMEM((LAG + 1, rows, model), bf16),
            ),
            in_specs=[hbm] * 6,
            out_specs=(vmem, vmem, vmem),
            scratch_shapes=[
                pltpu.VMEM((2, token_count), jnp.int32),
                pltpu.VMEM((1, token_count), jnp.int32),
                pltpu.VMEM((token_count, model), bf16),
                pltpu.VMEM(w_gate.shape, bf16),
                pltpu.VMEM((2, model, hidden), bf16),
                pltpu.VMEM((2, hidden, model), bf16),
                pltpu.VMEM((2, rows, model), bf16),
                pltpu.VMEM((LAG, rows, model), bf16),
                pltpu.VMEM((RESULTS, rows, model), bf16),
                pltpu.VMEM((rows, token_count), bf16),
                pltpu.VMEM((rows, hidden), bf16),
                pltpu.VMEM((8, token_count), f32),
                dma((2,)),
                dma((model // TILE,)),
                dma,
                dma((2,)),
                dma((2,)),
                dma((2,)),
                dma((LAG,)),
                dma((RESULTS,)),
                dma((LAG + 1,)),
            ],
            compiler_params=pltpu.CompilerParams(
                collective_id=0, has_side_effects=True, vmem_limit_bytes=VMEM_A
            ),
        )(expert_ids[0].T, keep_second, tokens, w_gate, w_in, w_out)
        return pl.pallas_call(
            functools.partial(last_kernel, (local - 1) * rows),
            out_shape=jax.ShapeDtypeStruct(tokens.shape, bf16),
            in_specs=[vmem, vmem, vmem],
            out_specs=hbm,
            scratch_shapes=[pltpu.VMEM((token_count, model), bf16), dma],
            compiler_params=pltpu.CompilerParams(vmem_limit_bytes=VMEM_B),
        )(acc, colb, yrecv)

    group_spec = P(("dp", "ep"))
    return jax.shard_map(
        local_layer,
        mesh=mesh,
        in_specs=(group_spec, P(), group_spec, group_spec, P("ep"), P("ep")),
        out_specs=group_spec,
        check_vma=False,
    )
```

```python
import functools

import jax
import jax.numpy as jnp
from jax import lax
from jax.experimental import pallas as pl
from jax.experimental.pallas import tpu as pltpu
from jax.sharding import PartitionSpec as P

MESH = pl.DeviceIdType.MESH
LAG = 3
TILE = 256
PIECE = 256
VMEM_A = 36 * 1024 * 1024
VMEM_B = 12 * 1024 * 1024


def ring_offsets(chip_count):
    near = sorted(range(1, chip_count), key=lambda d: min(d, chip_count - d))
    return near


def mix_weights(colb, base, rows, toks):
    base = jnp.int32(base).astype(jnp.float32)
    c1, c2 = colb[0, toks, :] - base, colb[1, toks, :] - base
    w1, w2 = colb[2, toks, :], colb[3, toks, :]
    parts = []
    for lane in range(0, rows, 128):
        want = (lax.broadcasted_iota(jnp.int32, (TILE, 128), 1) + lane).astype(jnp.float32)
        parts.append((jnp.where(c1 == want, w1, 0.0) + jnp.where(c2 == want, w2, 0.0)).astype(jnp.bfloat16))
    return jnp.concatenate(parts, axis=1)


def last_kernel(slot, acc, mix_last, yrecv, out_hbm, stage, sem):
    tokens, model = acc.shape

    def out_copy(i):
        toks = pl.ds(pl.multiple_of(i * TILE, TILE), TILE)
        return pltpu.make_async_copy(stage.at[toks], out_hbm.at[0, toks], sem)

    @pl.loop(0, tokens // TILE)
    def _(i):
        toks = pl.ds(pl.multiple_of(i * TILE, TILE), TILE)
        for j in range(0, model, 2 * TILE):
            cols = pl.ds(j, 2 * TILE)
            got = acc[toks, cols] + jnp.dot(mix_last[toks, :], yrecv[slot, :, cols], preferred_element_type=jnp.float32)
            stage[toks, cols] = got.astype(jnp.bfloat16)
        out_copy(i).start()

    pltpu.make_async_copy(stage, out_hbm.at[0], sem).wait()


def moe_kernel(
    n, sizes, ids_hbm, keep_hbm, x_hbm, wg_hbm, win_hbm, wout_hbm,
    acc, mix_last, yrecv,
    ids_ref, keep_ref, x_v, wg_v, win_v, wout_v, fsend, frecv, ysend, dmat, hid, crow, colb,
    id_sem, x_sem, wg_sem, win_sem, wout_sem, fs_sem, fr_sem, ys_sem, yr_sem,
):
    tokens, model, hidden, experts, local, capacity = sizes
    rows = n * capacity
    fslots, yslots = frecv.shape[0], yrecv.shape[0]
    shift = (local - 1).bit_length()
    blocks = tokens // TILE
    me = lax.axis_index("ep")

    def x_copy(j):
        cols = pl.ds(pl.multiple_of(j * TILE, TILE), TILE)
        return pltpu.make_async_copy(x_hbm.at[0, :, cols], x_v.at[:, cols], x_sem.at[j])

    id_copies = (
        pltpu.make_async_copy(ids_hbm, ids_ref, id_sem.at[0]),
        pltpu.make_async_copy(keep_hbm, keep_ref, id_sem.at[1]),
    )
    wg_copy = pltpu.make_async_copy(wg_hbm, wg_v, wg_sem)

    def weight_copies(k):
        b = lax.rem(k, 2)
        return (
            pltpu.make_async_copy(win_hbm.at[k], win_v.at[b], win_sem.at[b]),
            pltpu.make_async_copy(wout_hbm.at[k], wout_v.at[b], wout_sem.at[b]),
        )

    def owner_rows(d):
        return pl.ds(pl.multiple_of(d * capacity, capacity), capacity)

    cores = 2 if n % 2 == 0 else 1
    chips = n // cores
    my_chip, my_core = me // cores, lax.rem(me, cores)
    targets = []
    for dist in ring_offsets(chips) + [0]:
        for c in range(cores):
            if dist == 0 and c == 0:
                continue
            targets.append(lax.rem(my_chip + dist, chips) * cores + lax.rem(my_core + c, cores))

    def send(src, src_slot, dst, dst_slot, s_sem, r_sem, cols=slice(None)):
        for d in targets:
            pltpu.make_async_remote_copy(
                src_ref=src.at[src_slot, owner_rows(d), cols],
                dst_ref=dst.at[dst_slot, owner_rows(me), cols],
                send_sem=s_sem.at[src_slot],
                recv_sem=r_sem.at[dst_slot],
                device_id={"ep": d},
                device_id_type=MESH,
            ).start()

    def all_peers(src, src_slot, dst, dst_slot, s_sem, r_sem):
        part = pl.ds(0, (n - 1) * capacity)
        return pltpu.make_async_remote_copy(
            src_ref=src.at[src_slot, part],
            dst_ref=dst.at[dst_slot, part],
            send_sem=s_sem.at[src_slot],
            recv_sem=r_sem.at[dst_slot],
            device_id={"ep": me},
            device_id_type=MESH,
        )

    def fwd_args(k):
        return (fsend, lax.rem(k, 2), frecv, lax.rem(k, fslots), fs_sem, fr_sem)

    def back_args(k):
        return (ysend, lax.rem(k, 2), yrecv, lax.rem(k, yslots), ys_sem, yr_sem)

    def keep_own(src, src_slot, dst, dst_slot, *_):
        dst[dst_slot, owner_rows(me), :] = src[src_slot, owner_rows(me), :]

    def hot(blk, expert_row):
        return lax.broadcasted_iota(jnp.int32, (experts, TILE), 0) == expert_row

    def load_ids(b):
        cols = pl.ds(b * TILE, TILE)
        return ids_ref[0:1, cols], ids_ref[1:2, cols], keep_ref[0:1, cols] == 1

    def route(on_block):
        count = jnp.zeros((experts, TILE), jnp.float32)
        for b in range(blocks):
            i1, _, _ = load_ids(b)
            count = count + hot(b, i1).astype(jnp.float32)
        base1 = jnp.zeros((experts, 1), jnp.float32)
        base2 = jnp.sum(count, axis=1, keepdims=True)
        before = (
            lax.broadcasted_iota(jnp.int32, (TILE, TILE), 0) < lax.broadcasted_iota(jnp.int32, (TILE, TILE), 1)
        ).astype(jnp.bfloat16)
        for b in range(blocks):
            on_block(b)
            i1, i2, k2 = load_ids(b)
            hot1 = hot(b, i1).astype(jnp.float32)
            hot2 = jnp.where(k2, hot(b, i2).astype(jnp.float32), 0.0)
            ahead1 = jnp.dot(hot1.astype(jnp.bfloat16), before, preferred_element_type=jnp.float32) + base1
            ahead2 = jnp.dot(hot2.astype(jnp.bfloat16), before, preferred_element_type=jnp.float32) + base2
            base1 = base1 + jnp.sum(hot1, axis=1, keepdims=True)
            base2 = base2 + jnp.sum(hot2, axis=1, keepdims=True)
            pos1 = jnp.sum(ahead1 * hot1, axis=0, keepdims=True)
            pos2 = jnp.sum(ahead2 * hot2, axis=0, keepdims=True)

            def code(e, pos, kept):
                home = (e & (local - 1)) * rows + (e >> shift) * capacity
                return jnp.where(kept, home.astype(jnp.float32) + pos, -1.0)

            cols = pl.ds(b * TILE, TILE)
            crow[0:1, cols] = code(i1, pos1, pos1 < capacity)
            crow[1:2, cols] = code(i2, pos2, jnp.logical_and(k2, pos2 < capacity))

    def gates():
        for b in range(blocks):
            cols = pl.ds(b * TILE, TILE)
            i1, i2, k2 = load_ids(b)
            logits = jnp.dot(x_v[cols, :], wg_v[...], preferred_element_type=jnp.float32).T
            top = jnp.max(logits, axis=0, keepdims=True)
            grown = jnp.exp(logits - top)
            probs = grown / jnp.sum(grown, axis=0, keepdims=True)
            g1 = jnp.sum(jnp.where(hot(b, i1), probs, 0.0), axis=0, keepdims=True)
            g2 = jnp.where(k2, jnp.sum(jnp.where(hot(b, i2), probs, 0.0), axis=0, keepdims=True), 0.0)
            total = g1 + g2
            for q, row in enumerate((crow[0:1, cols], crow[1:2, cols], g1 / total, g2 / total)):
                colb[q, cols, :] = jnp.broadcast_to(row, (128, TILE)).T

    def dispatch_mask(k):
        base = (k * rows).astype(jnp.float32)
        for b in range(blocks):
            cols = pl.ds(b * TILE, TILE)
            want = lax.broadcasted_iota(jnp.int32, (rows, TILE), 0).astype(jnp.float32)
            c1, c2 = crow[0:1, cols] - base, crow[1:2, cols] - base
            dmat[:, cols] = jnp.where(jnp.logical_or(c1 == want, c2 == want), 1.0, 0.0).astype(jnp.bfloat16)

    def dispatch_tile(slot, j):
        cols = pl.ds(pl.multiple_of(j * TILE, TILE), TILE)
        fsend[slot, :, cols] = jnp.dot(dmat[...], x_v[:, cols], preferred_element_type=jnp.float32).astype(jnp.bfloat16)

    def dispatch(k):
        dispatch_mask(k)

        @pl.loop(0, model // TILE)
        def _(j):
            dispatch_tile(lax.rem(k, 2), j)

    def experts_ffn(k):
        w, slot, out_slot = lax.rem(k, 2), lax.rem(k, fslots), lax.rem(k, 2)

        @pl.loop(0, hidden // TILE)
        def _(j):
            cols = pl.ds(pl.multiple_of(j * TILE, TILE), TILE)
            h = jnp.dot(frecv[slot], win_v[w, :, cols], preferred_element_type=jnp.float32)
            hid[:, cols] = jnp.maximum(h, 0.0).astype(jnp.bfloat16)

        @pl.loop(0, model // TILE)
        def _(j):
            cols = pl.ds(pl.multiple_of(j * TILE, TILE), TILE)
            y = jnp.dot(hid[...], wout_v[w, :, cols], preferred_element_type=jnp.float32)
            ysend[out_slot, :, cols] = y.astype(jnp.bfloat16)

    def combine(k):
        @pl.loop(0, blocks)
        def _(i):
            toks = pl.ds(pl.multiple_of(i * TILE, TILE), TILE)
            mix = mix_weights(colb, k * rows, rows, toks)
            for j in range(0, model, 2 * TILE):
                cols = pl.ds(j, 2 * TILE)
                acc[toks, cols] += jnp.dot(
                    mix, yrecv[lax.rem(k, yslots), :, cols], preferred_element_type=jnp.float32
                )

    for copy in id_copies:
        copy.start()
    x_copy(0).start()
    barrier = pltpu.get_barrier_semaphore()
    for d in targets:
        pl.semaphore_signal(barrier, inc=1, device_id={"ep": d}, device_id_type=MESH)
    for copy in id_copies:
        copy.wait()
    tiles = model // TILE
    ahead = min(4, tiles - 1)

    def next_tile(b):
        if b % 2 == 0 and 1 + b // 2 <= ahead:
            x_copy(1 + b // 2).start()

    route(next_tile)
    first = jnp.int32(0)
    dispatch_mask(first)
    pl.semaphore_wait(barrier, n - 1)

    @pl.loop(0, model // PIECE)
    def _(piece):
        for j in range(PIECE // TILE):
            tile = piece * (PIECE // TILE) + j
            x_copy(tile).wait()

            @pl.when(tile + ahead + 1 < tiles)
            def _():
                x_copy(tile + ahead + 1).start()

            dispatch_tile(0, tile)
        send(*fwd_args(first), pl.ds(pl.multiple_of(piece * PIECE, PIECE), PIECE))

    keep_own(*fwd_args(first))
    wg_copy.start()
    for copy in weight_copies(first):
        copy.start()

    @pl.loop(0, local + LAG)
    def _(t):
        @pl.when(t >= LAG)
        def _():
            all_peers(*back_args(t - LAG)).wait_recv()

        @pl.when(jnp.logical_and(t >= 1, t < local))
        def _():
            send(*fwd_args(t))
            keep_own(*fwd_args(t))

        @pl.when(t == 1)
        def _():
            wg_copy.wait()
            gates()

            @pl.loop(0, blocks)
            def _(i):
                acc[pl.ds(pl.multiple_of(i * TILE, TILE), TILE), :] = jnp.zeros((TILE, model), jnp.float32)

        @pl.when(jnp.logical_and(t >= LAG, t < local + LAG - 1))
        def _():
            combine(t - LAG)

        @pl.when(t == local)
        def _():
            @pl.loop(0, blocks)
            def _(i):
                toks = pl.ds(pl.multiple_of(i * TILE, TILE), TILE)
                mix_last[toks, :] = mix_weights(colb, (local - 1) * rows, rows, toks)

        @pl.when(jnp.logical_and(t >= 1, t <= local))
        def _():
            k = t - 1

            @pl.when(t < local)
            def _():
                for copy in weight_copies(t):
                    copy.start()

            for copy in weight_copies(k):
                copy.wait()
            all_peers(*fwd_args(k)).wait_recv()

            @pl.when(k >= 2)
            def _():
                all_peers(*back_args(k - 2)).wait_send()

            experts_ffn(k)
            send(*back_args(k))
            keep_own(*back_args(k))

        @pl.when(t + 1 < local)
        def _():
            @pl.when(t >= 1)
            def _():
                all_peers(*fwd_args(t - 1)).wait_send()

            dispatch(t + 1)

    for k in range(max(local - 2, 0), local):
        all_peers(*fwd_args(jnp.int32(k))).wait_send()
        all_peers(*back_args(jnp.int32(k))).wait_send()


def solution(mesh):
    n = mesh.shape["ep"]

    def local_layer(tokens, w_gate, expert_ids, keep_second, w_in, w_out):
        _, token_count, model = tokens.shape
        experts = w_gate.shape[1]
        local, _, hidden = w_in.shape
        capacity = 2 * token_count // experts
        rows = n * capacity
        bf16, f32 = jnp.bfloat16, jnp.float32
        sizes = (token_count, model, hidden, experts, local, capacity)
        vmem, hbm = pl.BlockSpec(memory_space=pltpu.VMEM), pl.BlockSpec(memory_space=pl.ANY)
        dma = pltpu.SemaphoreType.DMA
        acc, mix_last, yrecv = pl.pallas_call(
            functools.partial(moe_kernel, n, sizes),
            out_shape=(
                pltpu.VMEM((token_count, model), f32),
                pltpu.VMEM((token_count, rows), bf16),
                pltpu.VMEM((LAG + 1, rows, model), bf16),
            ),
            in_specs=[hbm] * 6,
            out_specs=(vmem, vmem, vmem),
            scratch_shapes=[
                pltpu.VMEM((2, token_count), jnp.int32),
                pltpu.VMEM((1, token_count), jnp.int32),
                pltpu.VMEM((token_count, model), bf16),
                pltpu.VMEM(w_gate.shape, bf16),
                pltpu.VMEM((2, model, hidden), bf16),
                pltpu.VMEM((2, hidden, model), bf16),
                pltpu.VMEM((2, rows, model), bf16),
                pltpu.VMEM((LAG, rows, model), bf16),
                pltpu.VMEM((2, rows, model), bf16),
                pltpu.VMEM((rows, token_count), bf16),
                pltpu.VMEM((rows, hidden), bf16),
                pltpu.VMEM((8, token_count), f32),
                pltpu.VMEM((4, token_count, 128), f32),
                dma((2,)),
                dma((model // TILE,)),
                dma,
                dma((2,)),
                dma((2,)),
                dma((2,)),
                dma((LAG,)),
                dma((2,)),
                dma((LAG + 1,)),
            ],
            compiler_params=pltpu.CompilerParams(
                collective_id=0, has_side_effects=True, vmem_limit_bytes=VMEM_A
            ),
        )(expert_ids[0].T, keep_second, tokens, w_gate, w_in, w_out)
        return pl.pallas_call(
            functools.partial(last_kernel, (local - 1) % (LAG + 1)),
            out_shape=jax.ShapeDtypeStruct(tokens.shape, bf16),
            in_specs=[vmem, vmem, vmem],
            out_specs=hbm,
            scratch_shapes=[pltpu.VMEM((token_count, model), bf16), dma],
            compiler_params=pltpu.CompilerParams(vmem_limit_bytes=VMEM_B),
        )(acc, mix_last, yrecv)

    group_spec = P(("dp", "ep"))
    return jax.shard_map(
        local_layer,
        mesh=mesh,
        in_specs=(group_spec, P(), group_spec, group_spec, P("ep"), P("ep")),
        out_specs=group_spec,
        check_vma=False,
    )
```

```python
import functools

import jax
import jax.numpy as jnp
from jax import lax
from jax.experimental import pallas as pl
from jax.experimental.pallas import tpu as pltpu
from jax.sharding import PartitionSpec as P

MESH = pl.DeviceIdType.MESH
LAG = 3
TILE = 256
PIECE = 256
VMEM_A = 36 * 1024 * 1024
VMEM_B = 12 * 1024 * 1024


def ring_offsets(chip_count):
    return sorted(range(1, chip_count), key=lambda d: -min(d, chip_count - d))


def mix_weights(colb, base, rows, toks):
    base = jnp.int32(base).astype(jnp.float32)
    c1, c2 = colb[0, toks, :] - base, colb[1, toks, :] - base
    w1, w2 = colb[2, toks, :], colb[3, toks, :]
    parts = []
    for lane in range(0, rows, 128):
        want = (lax.broadcasted_iota(jnp.int32, (TILE, 128), 1) + lane).astype(jnp.float32)
        parts.append((jnp.where(c1 == want, w1, 0.0) + jnp.where(c2 == want, w2, 0.0)).astype(jnp.bfloat16))
    return jnp.concatenate(parts, axis=1)


def last_kernel(slot, acc, mix_last, yrecv, out_hbm, stage, sem):
    tokens, model = acc.shape

    def out_copy(i):
        toks = pl.ds(pl.multiple_of(i * TILE, TILE), TILE)
        return pltpu.make_async_copy(stage.at[toks], out_hbm.at[0, toks], sem)

    @pl.loop(0, tokens // TILE)
    def _(i):
        toks = pl.ds(pl.multiple_of(i * TILE, TILE), TILE)
        for j in range(0, model, 2 * TILE):
            cols = pl.ds(j, 2 * TILE)
            got = acc[toks, cols] + jnp.dot(mix_last[toks, :], yrecv[slot, :, cols], preferred_element_type=jnp.float32)
            stage[toks, cols] = got.astype(jnp.bfloat16)
        out_copy(i).start()

    pltpu.make_async_copy(stage, out_hbm.at[0], sem).wait()


def moe_kernel(
    n, sizes, ids_hbm, keep_hbm, x_hbm, wg_hbm, win_hbm, wout_hbm,
    acc, mix_last, yrecv,
    ids_ref, keep_ref, x_v, wg_v, win_v, wout_v, fsend, frecv, ysend, dmat, hid, crow, colb,
    id_sem, x_sem, wg_sem, win_sem, wout_sem, fs_sem, fr_sem, ys_sem, yr_sem,
):
    tokens, model, hidden, experts, local, capacity = sizes
    rows = n * capacity
    fslots, yslots = frecv.shape[0], yrecv.shape[0]
    shift = (local - 1).bit_length()
    blocks = tokens // TILE
    me = lax.axis_index("ep")

    def x_copy(j):
        cols = pl.ds(pl.multiple_of(j * TILE, TILE), TILE)
        return pltpu.make_async_copy(x_hbm.at[0, :, cols], x_v.at[:, cols], x_sem.at[j])

    id_copies = (
        pltpu.make_async_copy(ids_hbm, ids_ref, id_sem.at[0]),
        pltpu.make_async_copy(keep_hbm, keep_ref, id_sem.at[1]),
    )
    wg_copy = pltpu.make_async_copy(wg_hbm, wg_v, wg_sem)

    def weight_copies(k):
        b = lax.rem(k, 2)
        return (
            pltpu.make_async_copy(win_hbm.at[k], win_v.at[b], win_sem.at[b]),
            pltpu.make_async_copy(wout_hbm.at[k], wout_v.at[b], wout_sem.at[b]),
        )

    def owner_rows(d):
        return pl.ds(pl.multiple_of(d * capacity, capacity), capacity)

    cores = 2 if n % 2 == 0 else 1
    chips = n // cores
    my_chip, my_core = me // cores, lax.rem(me, cores)
    targets = []
    for dist in ring_offsets(chips) + [0]:
        for c in range(cores):
            if dist == 0 and c == 0:
                continue
            targets.append(lax.rem(my_chip + dist, chips) * cores + lax.rem(my_core + c, cores))

    def send(src, src_slot, dst, dst_slot, s_sem, r_sem, cols=slice(None)):
        for d in targets:
            pltpu.make_async_remote_copy(
                src_ref=src.at[src_slot, owner_rows(d), cols],
                dst_ref=dst.at[dst_slot, owner_rows(me), cols],
                send_sem=s_sem.at[src_slot],
                recv_sem=r_sem.at[dst_slot],
                device_id={"ep": d},
                device_id_type=MESH,
            ).start()

    def all_peers(src, src_slot, dst, dst_slot, s_sem, r_sem):
        part = pl.ds(0, (n - 1) * capacity)
        return pltpu.make_async_remote_copy(
            src_ref=src.at[src_slot, part],
            dst_ref=dst.at[dst_slot, part],
            send_sem=s_sem.at[src_slot],
            recv_sem=r_sem.at[dst_slot],
            device_id={"ep": me},
            device_id_type=MESH,
        )

    def fwd_args(k):
        return (fsend, lax.rem(k, 2), frecv, lax.rem(k, fslots), fs_sem, fr_sem)

    def back_args(k):
        return (ysend, lax.rem(k, 2), yrecv, lax.rem(k, yslots), ys_sem, yr_sem)

    def keep_own(src, src_slot, dst, dst_slot, *_):
        dst[dst_slot, owner_rows(me), :] = src[src_slot, owner_rows(me), :]

    def hot(blk, expert_row):
        return lax.broadcasted_iota(jnp.int32, (experts, TILE), 0) == expert_row

    def load_ids(b):
        cols = pl.ds(b * TILE, TILE)
        return ids_ref[0:1, cols], ids_ref[1:2, cols], keep_ref[0:1, cols] == 1

    def route(on_block):
        count = jnp.zeros((experts, TILE), jnp.float32)
        for b in range(blocks):
            i1, _, _ = load_ids(b)
            count = count + hot(b, i1).astype(jnp.float32)
        base1 = jnp.zeros((experts, 1), jnp.float32)
        base2 = jnp.sum(count, axis=1, keepdims=True)
        before = (
            lax.broadcasted_iota(jnp.int32, (TILE, TILE), 0) < lax.broadcasted_iota(jnp.int32, (TILE, TILE), 1)
        ).astype(jnp.bfloat16)
        for b in range(blocks):
            on_block(b)
            i1, i2, k2 = load_ids(b)
            hot1 = hot(b, i1).astype(jnp.float32)
            hot2 = jnp.where(k2, hot(b, i2).astype(jnp.float32), 0.0)
            ahead1 = jnp.dot(hot1.astype(jnp.bfloat16), before, preferred_element_type=jnp.float32) + base1
            ahead2 = jnp.dot(hot2.astype(jnp.bfloat16), before, preferred_element_type=jnp.float32) + base2
            base1 = base1 + jnp.sum(hot1, axis=1, keepdims=True)
            base2 = base2 + jnp.sum(hot2, axis=1, keepdims=True)
            pos1 = jnp.sum(ahead1 * hot1, axis=0, keepdims=True)
            pos2 = jnp.sum(ahead2 * hot2, axis=0, keepdims=True)

            def code(e, pos, kept):
                home = (e & (local - 1)) * rows + (e >> shift) * capacity
                return jnp.where(kept, home.astype(jnp.float32) + pos, -1.0)

            cols = pl.ds(b * TILE, TILE)
            crow[0:1, cols] = code(i1, pos1, pos1 < capacity)
            crow[1:2, cols] = code(i2, pos2, jnp.logical_and(k2, pos2 < capacity))

    def gates():
        for b in range(blocks):
            cols = pl.ds(b * TILE, TILE)
            i1, i2, k2 = load_ids(b)
            logits = jnp.dot(x_v[cols, :], wg_v[...], preferred_element_type=jnp.float32).T
            top = jnp.max(logits, axis=0, keepdims=True)
            grown = jnp.exp(logits - top)
            probs = grown / jnp.sum(grown, axis=0, keepdims=True)
            g1 = jnp.sum(jnp.where(hot(b, i1), probs, 0.0), axis=0, keepdims=True)
            g2 = jnp.where(k2, jnp.sum(jnp.where(hot(b, i2), probs, 0.0), axis=0, keepdims=True), 0.0)
            total = g1 + g2
            for q, row in enumerate((crow[0:1, cols], crow[1:2, cols], g1 / total, g2 / total)):
                colb[q, cols, :] = jnp.broadcast_to(row, (128, TILE)).T

    def dispatch_mask(k):
        base = (k * rows).astype(jnp.float32)
        for b in range(blocks):
            cols = pl.ds(b * TILE, TILE)
            want = lax.broadcasted_iota(jnp.int32, (rows, TILE), 0).astype(jnp.float32)
            c1, c2 = crow[0:1, cols] - base, crow[1:2, cols] - base
            dmat[:, cols] = jnp.where(jnp.logical_or(c1 == want, c2 == want), 1.0, 0.0).astype(jnp.bfloat16)

    def dispatch_tile(slot, j):
        cols = pl.ds(pl.multiple_of(j * TILE, TILE), TILE)
        fsend[slot, :, cols] = jnp.dot(dmat[...], x_v[:, cols], preferred_element_type=jnp.float32).astype(jnp.bfloat16)

    def dispatch(k):
        dispatch_mask(k)

        @pl.loop(0, model // TILE)
        def _(j):
            dispatch_tile(lax.rem(k, 2), j)

    def experts_ffn(k):
        w, slot, out_slot = lax.rem(k, 2), lax.rem(k, fslots), lax.rem(k, 2)

        @pl.loop(0, hidden // TILE)
        def _(j):
            cols = pl.ds(pl.multiple_of(j * TILE, TILE), TILE)
            h = jnp.dot(frecv[slot], win_v[w, :, cols], preferred_element_type=jnp.float32)
            hid[:, cols] = jnp.maximum(h, 0.0).astype(jnp.bfloat16)

        @pl.loop(0, model // TILE)
        def _(j):
            cols = pl.ds(pl.multiple_of(j * TILE, TILE), TILE)
            y = jnp.dot(hid[...], wout_v[w, :, cols], preferred_element_type=jnp.float32)
            ysend[out_slot, :, cols] = y.astype(jnp.bfloat16)

    def combine(k):
        @pl.loop(0, blocks)
        def _(i):
            toks = pl.ds(pl.multiple_of(i * TILE, TILE), TILE)
            mix = mix_weights(colb, k * rows, rows, toks)
            for j in range(0, model, 2 * TILE):
                cols = pl.ds(j, 2 * TILE)
                acc[toks, cols] += jnp.dot(
                    mix, yrecv[lax.rem(k, yslots), :, cols], preferred_element_type=jnp.float32
                )

    for copy in id_copies:
        copy.start()
    x_copy(0).start()
    barrier = pltpu.get_barrier_semaphore()
    for d in targets:
        pl.semaphore_signal(barrier, inc=1, device_id={"ep": d}, device_id_type=MESH)
    for copy in id_copies:
        copy.wait()
    tiles = model // TILE
    ahead = min(4, tiles - 1)

    def next_tile(b):
        if b % 2 == 0 and 1 + b // 2 <= ahead:
            x_copy(1 + b // 2).start()

    route(next_tile)
    first = jnp.int32(0)
    dispatch_mask(first)
    pl.semaphore_wait(barrier, n - 1)

    @pl.loop(0, model // PIECE)
    def _(piece):
        for j in range(PIECE // TILE):
            tile = piece * (PIECE // TILE) + j
            x_copy(tile).wait()

            @pl.when(tile + ahead + 1 < tiles)
            def _():
                x_copy(tile + ahead + 1).start()

            dispatch_tile(0, tile)
        send(*fwd_args(first), pl.ds(pl.multiple_of(piece * PIECE, PIECE), PIECE))

    keep_own(*fwd_args(first))
    wg_copy.start()
    for copy in weight_copies(first):
        copy.start()

    @pl.loop(0, local + LAG)
    def _(t):
        @pl.when(t >= LAG)
        def _():
            all_peers(*back_args(t - LAG)).wait_recv()

        @pl.when(jnp.logical_and(t >= 1, t < local))
        def _():
            send(*fwd_args(t))
            keep_own(*fwd_args(t))

        @pl.when(t == 1)
        def _():
            wg_copy.wait()
            gates()

            @pl.loop(0, blocks)
            def _(i):
                acc[pl.ds(pl.multiple_of(i * TILE, TILE), TILE), :] = jnp.zeros((TILE, model), jnp.float32)

        @pl.when(jnp.logical_and(t >= LAG, t < local + LAG - 1))
        def _():
            combine(t - LAG)

        @pl.when(t == local)
        def _():
            @pl.loop(0, blocks)
            def _(i):
                toks = pl.ds(pl.multiple_of(i * TILE, TILE), TILE)
                mix_last[toks, :] = mix_weights(colb, (local - 1) * rows, rows, toks)

        @pl.when(jnp.logical_and(t >= 1, t <= local))
        def _():
            k = t - 1

            @pl.when(t < local)
            def _():
                for copy in weight_copies(t):
                    copy.start()

            for copy in weight_copies(k):
                copy.wait()
            all_peers(*fwd_args(k)).wait_recv()

            @pl.when(k >= 2)
            def _():
                all_peers(*back_args(k - 2)).wait_send()

            experts_ffn(k)
            send(*back_args(k))
            keep_own(*back_args(k))

        @pl.when(t + 1 < local)
        def _():
            @pl.when(t >= 1)
            def _():
                all_peers(*fwd_args(t - 1)).wait_send()

            dispatch(t + 1)

    for k in range(max(local - 2, 0), local):
        all_peers(*fwd_args(jnp.int32(k))).wait_send()
        all_peers(*back_args(jnp.int32(k))).wait_send()


def solution(mesh):
    n = mesh.shape["ep"]

    def local_layer(tokens, w_gate, expert_ids, keep_second, w_in, w_out):
        _, token_count, model = tokens.shape
        experts = w_gate.shape[1]
        local, _, hidden = w_in.shape
        capacity = 2 * token_count // experts
        rows = n * capacity
        bf16, f32 = jnp.bfloat16, jnp.float32
        sizes = (token_count, model, hidden, experts, local, capacity)
        vmem, hbm = pl.BlockSpec(memory_space=pltpu.VMEM), pl.BlockSpec(memory_space=pl.ANY)
        dma = pltpu.SemaphoreType.DMA
        acc, mix_last, yrecv = pl.pallas_call(
            functools.partial(moe_kernel, n, sizes),
            out_shape=(
                pltpu.VMEM((token_count, model), f32),
                pltpu.VMEM((token_count, rows), bf16),
                pltpu.VMEM((LAG + 1, rows, model), bf16),
            ),
            in_specs=[hbm] * 6,
            out_specs=(vmem, vmem, vmem),
            scratch_shapes=[
                pltpu.VMEM((2, token_count), jnp.int32),
                pltpu.VMEM((1, token_count), jnp.int32),
                pltpu.VMEM((token_count, model), bf16),
                pltpu.VMEM(w_gate.shape, bf16),
                pltpu.VMEM((2, model, hidden), bf16),
                pltpu.VMEM((2, hidden, model), bf16),
                pltpu.VMEM((2, rows, model), bf16),
                pltpu.VMEM((LAG, rows, model), bf16),
                pltpu.VMEM((2, rows, model), bf16),
                pltpu.VMEM((rows, token_count), bf16),
                pltpu.VMEM((rows, hidden), bf16),
                pltpu.VMEM((8, token_count), f32),
                pltpu.VMEM((4, token_count, 128), f32),
                dma((2,)),
                dma((model // TILE,)),
                dma,
                dma((2,)),
                dma((2,)),
                dma((2,)),
                dma((LAG,)),
                dma((2,)),
                dma((LAG + 1,)),
            ],
            compiler_params=pltpu.CompilerParams(
                collective_id=0, has_side_effects=True, vmem_limit_bytes=VMEM_A
            ),
        )(expert_ids[0].T, keep_second, tokens, w_gate, w_in, w_out)
        return pl.pallas_call(
            functools.partial(last_kernel, (local - 1) % (LAG + 1)),
            out_shape=jax.ShapeDtypeStruct(tokens.shape, bf16),
            in_specs=[vmem, vmem, vmem],
            out_specs=hbm,
            scratch_shapes=[pltpu.VMEM((token_count, model), bf16), dma],
            compiler_params=pltpu.CompilerParams(vmem_limit_bytes=VMEM_B),
        )(acc, mix_last, yrecv)

    group_spec = P(("dp", "ep"))
    return jax.shard_map(
        local_layer,
        mesh=mesh,
        in_specs=(group_spec, P(), group_spec, group_spec, P("ep"), P("ep")),
        out_specs=group_spec,
        check_vma=False,
    )
```

```python
import functools

import jax
import jax.numpy as jnp
from jax import lax
from jax.experimental import pallas as pl
from jax.experimental.pallas import tpu as pltpu
from jax.sharding import PartitionSpec as P

MESH = pl.DeviceIdType.MESH
LAG = 3
TILE = 256
PIECE = 256
VMEM_A = 36 * 1024 * 1024
VMEM_B = 12 * 1024 * 1024


def ring_offsets(chip_count):
    return sorted(range(1, chip_count), key=lambda d: -min(d, chip_count - d))


def mix_weights(colb, base, rows, toks):
    base = jnp.int32(base).astype(jnp.float32)
    c1, c2 = colb[0, toks, :] - base, colb[1, toks, :] - base
    w1, w2 = colb[2, toks, :], colb[3, toks, :]
    parts = []
    for lane in range(0, rows, 128):
        want = (lax.broadcasted_iota(jnp.int32, (TILE, 128), 1) + lane).astype(jnp.float32)
        parts.append((jnp.where(c1 == want, w1, 0.0) + jnp.where(c2 == want, w2, 0.0)).astype(jnp.bfloat16))
    return jnp.concatenate(parts, axis=1)


def last_kernel(slot, acc, mix_last, yrecv, out_hbm, stage, sem):
    tokens, model = acc.shape

    def out_copy(i):
        toks = pl.ds(pl.multiple_of(i * TILE, TILE), TILE)
        return pltpu.make_async_copy(stage.at[toks], out_hbm.at[0, toks], sem)

    @pl.loop(0, tokens // TILE)
    def _(i):
        toks = pl.ds(pl.multiple_of(i * TILE, TILE), TILE)
        for j in range(0, model, 2 * TILE):
            cols = pl.ds(j, 2 * TILE)
            got = acc[toks, cols] + jnp.dot(mix_last[toks, :], yrecv[slot, :, cols], preferred_element_type=jnp.float32)
            stage[toks, cols] = got.astype(jnp.bfloat16)
        out_copy(i).start()

    pltpu.make_async_copy(stage, out_hbm.at[0], sem).wait()


def moe_kernel(
    n, sizes, ids_hbm, keep_hbm, x_hbm, wg_hbm, win_hbm, wout_hbm,
    acc, mix_last, yrecv,
    ids_ref, keep_ref, x_v, wg_v, win_v, wout_v, fsend, frecv, ysend, dmat, hid, crow, colb,
    id_sem, x_sem, wg_sem, win_sem, wout_sem, fs_sem, fr_sem, ys_sem, yr_sem,
):
    tokens, model, hidden, experts, local, capacity = sizes
    rows = n * capacity
    fslots, yslots = frecv.shape[0], yrecv.shape[0]
    shift = (local - 1).bit_length()
    blocks = tokens // TILE
    me = lax.axis_index("ep")

    def x_copy(j):
        cols = pl.ds(pl.multiple_of(j * TILE, TILE), TILE)
        return pltpu.make_async_copy(x_hbm.at[0, :, cols], x_v.at[:, cols], x_sem.at[j])

    id_copies = (
        pltpu.make_async_copy(ids_hbm, ids_ref, id_sem.at[0]),
        pltpu.make_async_copy(keep_hbm, keep_ref, id_sem.at[1]),
    )
    wg_copy = pltpu.make_async_copy(wg_hbm, wg_v, wg_sem)

    def weight_copies(k):
        b = lax.rem(k, 2)
        return (
            pltpu.make_async_copy(win_hbm.at[k], win_v.at[b], win_sem.at[b]),
            pltpu.make_async_copy(wout_hbm.at[k], wout_v.at[b], wout_sem.at[b]),
        )

    def owner_rows(d):
        return pl.ds(pl.multiple_of(d * capacity, capacity), capacity)

    cores = 2 if n % 2 == 0 else 1
    chips = n // cores
    my_chip, my_core = me // cores, lax.rem(me, cores)
    targets = []
    for dist in ring_offsets(chips) + [0]:
        for c in range(cores):
            if dist == 0 and c == 0:
                continue
            targets.append(lax.rem(my_chip + dist, chips) * cores + lax.rem(my_core + c, cores))

    def send(src, src_slot, dst, dst_slot, s_sem, r_sem, cols=slice(None)):
        for d in targets:
            pltpu.make_async_remote_copy(
                src_ref=src.at[src_slot, owner_rows(d), cols],
                dst_ref=dst.at[dst_slot, owner_rows(me), cols],
                send_sem=s_sem.at[src_slot],
                recv_sem=r_sem.at[dst_slot],
                device_id={"ep": d},
                device_id_type=MESH,
            ).start()

    def all_peers(src, src_slot, dst, dst_slot, s_sem, r_sem):
        part = pl.ds(0, (n - 1) * capacity)
        return pltpu.make_async_remote_copy(
            src_ref=src.at[src_slot, part],
            dst_ref=dst.at[dst_slot, part],
            send_sem=s_sem.at[src_slot],
            recv_sem=r_sem.at[dst_slot],
            device_id={"ep": me},
            device_id_type=MESH,
        )

    def fwd_args(k):
        return (fsend, lax.rem(k, 2), frecv, lax.rem(k, fslots), fs_sem, fr_sem)

    def back_args(k):
        return (ysend, lax.rem(k, 2), yrecv, lax.rem(k, yslots), ys_sem, yr_sem)

    def keep_own(src, src_slot, dst, dst_slot, *_):
        dst[dst_slot, owner_rows(me), :] = src[src_slot, owner_rows(me), :]

    def hot(blk, expert_row):
        return lax.broadcasted_iota(jnp.int32, (experts, TILE), 0) == expert_row

    def load_ids(b):
        cols = pl.ds(b * TILE, TILE)
        return ids_ref[0:1, cols], ids_ref[1:2, cols], keep_ref[0:1, cols] == 1

    def route(on_block):
        bf16, f32 = jnp.bfloat16, jnp.float32
        expert = lax.broadcasted_iota(jnp.int32, (experts, TILE), 0)
        ones = jnp.ones((TILE, 128), bf16)
        order = lax.broadcasted_iota(jnp.int32, (TILE, TILE), 0) < lax.broadcasted_iota(jnp.int32, (TILE, TILE), 1)
        earlier = jnp.concatenate([jnp.where(order, 1.0, 0.0).astype(bf16), ones], axis=1)
        packed_expert = expert.astype(f32).astype(bf16)

        def one_hot(row):
            return jnp.where(packed_expert == row.astype(f32).astype(bf16), bf16(1), bf16(0))

        count = jnp.zeros((experts, TILE), bf16)
        for b in range(blocks):
            count = count + one_hot(load_ids(b)[0])
        base1 = jnp.zeros((experts, 128), f32)
        base2 = jnp.dot(count, ones, preferred_element_type=f32)
        for b in range(blocks):
            on_block(b)
            i1, i2, k2 = load_ids(b)
            kept2 = jnp.where(k2, i2, -1)
            hots = jnp.concatenate([one_hot(i1), one_hot(kept2)], axis=0)
            ahead = jnp.dot(hots, earlier, preferred_element_type=f32)
            ahead1, ahead2 = ahead[:experts], ahead[experts:]
            for lane in range(0, TILE, 128):
                part = slice(lane, lane + 128)
                cols = pl.ds(b * TILE + lane, 128)
                is1, is2 = expert[:, part] == i1[:, part], expert[:, part] == kept2[:, part]
                pos1 = jnp.sum(jnp.where(is1, ahead1[:, part] + base1, 0.0), axis=0, keepdims=True)
                pos2 = jnp.sum(jnp.where(is2, ahead2[:, part] + base2, 0.0), axis=0, keepdims=True)

                def code(e, pos, kept):
                    home = (e & (local - 1)) * rows + (e >> shift) * capacity
                    return jnp.where(kept, home.astype(f32) + pos, -1.0)

                crow[0:1, cols] = code(i1[:, part], pos1, pos1 < capacity)
                crow[1:2, cols] = code(i2[:, part], pos2, jnp.logical_and(k2[:, part], pos2 < capacity))
            base1 = base1 + ahead1[:, TILE:]
            base2 = base2 + ahead2[:, TILE:]

    def gates():
        for b in range(blocks):
            cols = pl.ds(b * TILE, TILE)
            i1, i2, k2 = load_ids(b)
            logits = jnp.dot(x_v[cols, :], wg_v[...], preferred_element_type=jnp.float32).T
            top = jnp.max(logits, axis=0, keepdims=True)
            grown = jnp.exp(logits - top)
            probs = grown / jnp.sum(grown, axis=0, keepdims=True)
            g1 = jnp.sum(jnp.where(hot(b, i1), probs, 0.0), axis=0, keepdims=True)
            g2 = jnp.where(k2, jnp.sum(jnp.where(hot(b, i2), probs, 0.0), axis=0, keepdims=True), 0.0)
            total = g1 + g2
            for q, row in enumerate((crow[0:1, cols], crow[1:2, cols], g1 / total, g2 / total)):
                colb[q, cols, :] = jnp.broadcast_to(row, (128, TILE)).T

    def dispatch_mask(k):
        base = (k * rows).astype(jnp.float32)
        want = lax.broadcasted_iota(jnp.int32, (rows, TILE), 0).astype(jnp.float32).astype(jnp.bfloat16)
        for b in range(blocks):
            cols = pl.ds(b * TILE, TILE)

            def row_of(q):
                row = crow[q : q + 1, cols] - base
                return jnp.where(jnp.logical_and(row >= 0.0, row < rows), row, -1.0).astype(jnp.bfloat16)

            hit = jnp.logical_or(want == row_of(0), want == row_of(1))
            dmat[:, cols] = jnp.where(hit, jnp.bfloat16(1), jnp.bfloat16(0))

    def dispatch_tile(slot, j):
        cols = pl.ds(pl.multiple_of(j * TILE, TILE), TILE)
        fsend[slot, :, cols] = jnp.dot(dmat[...], x_v[:, cols], preferred_element_type=jnp.float32).astype(jnp.bfloat16)

    def dispatch(k):
        dispatch_mask(k)

        @pl.loop(0, model // TILE)
        def _(j):
            dispatch_tile(lax.rem(k, 2), j)

    def experts_ffn(k):
        w, slot, out_slot = lax.rem(k, 2), lax.rem(k, fslots), lax.rem(k, 2)

        @pl.loop(0, hidden // TILE)
        def _(j):
            cols = pl.ds(pl.multiple_of(j * TILE, TILE), TILE)
            h = jnp.dot(frecv[slot], win_v[w, :, cols], preferred_element_type=jnp.float32)
            hid[:, cols] = jnp.maximum(h, 0.0).astype(jnp.bfloat16)

        @pl.loop(0, model // TILE)
        def _(j):
            cols = pl.ds(pl.multiple_of(j * TILE, TILE), TILE)
            y = jnp.dot(hid[...], wout_v[w, :, cols], preferred_element_type=jnp.float32)
            ysend[out_slot, :, cols] = y.astype(jnp.bfloat16)

    def combine(k):
        @pl.loop(0, blocks)
        def _(i):
            toks = pl.ds(pl.multiple_of(i * TILE, TILE), TILE)
            mix = mix_weights(colb, k * rows, rows, toks)
            for j in range(0, model, 2 * TILE):
                cols = pl.ds(j, 2 * TILE)
                acc[toks, cols] += jnp.dot(
                    mix, yrecv[lax.rem(k, yslots), :, cols], preferred_element_type=jnp.float32
                )

    for copy in id_copies:
        copy.start()
    x_copy(0).start()
    barrier = pltpu.get_barrier_semaphore()
    for d in targets:
        pl.semaphore_signal(barrier, inc=1, device_id={"ep": d}, device_id_type=MESH)
    for copy in id_copies:
        copy.wait()
    tiles = model // TILE
    ahead = min(4, tiles - 1)

    def next_tile(b):
        if b % 2 == 0 and 1 + b // 2 <= ahead:
            x_copy(1 + b // 2).start()

    route(next_tile)
    first = jnp.int32(0)
    dispatch_mask(first)
    pl.semaphore_wait(barrier, n - 1)

    @pl.loop(0, model // PIECE)
    def _(piece):
        for j in range(PIECE // TILE):
            tile = piece * (PIECE // TILE) + j
            x_copy(tile).wait()

            @pl.when(tile + ahead + 1 < tiles)
            def _():
                x_copy(tile + ahead + 1).start()

            dispatch_tile(0, tile)
        send(*fwd_args(first), pl.ds(pl.multiple_of(piece * PIECE, PIECE), PIECE))

    keep_own(*fwd_args(first))
    wg_copy.start()
    for copy in weight_copies(first):
        copy.start()

    @pl.loop(0, local + LAG)
    def _(t):
        @pl.when(t >= LAG)
        def _():
            all_peers(*back_args(t - LAG)).wait_recv()

        @pl.when(jnp.logical_and(t >= 1, t < local))
        def _():
            send(*fwd_args(t))
            keep_own(*fwd_args(t))

        @pl.when(t == 1)
        def _():
            wg_copy.wait()
            gates()

            @pl.loop(0, blocks)
            def _(i):
                acc[pl.ds(pl.multiple_of(i * TILE, TILE), TILE), :] = jnp.zeros((TILE, model), jnp.float32)

        @pl.when(jnp.logical_and(t >= LAG, t < local + LAG - 1))
        def _():
            combine(t - LAG)

        @pl.when(t == local)
        def _():
            @pl.loop(0, blocks)
            def _(i):
                toks = pl.ds(pl.multiple_of(i * TILE, TILE), TILE)
                mix_last[toks, :] = mix_weights(colb, (local - 1) * rows, rows, toks)

        @pl.when(jnp.logical_and(t >= 1, t <= local))
        def _():
            k = t - 1

            @pl.when(t < local)
            def _():
                for copy in weight_copies(t):
                    copy.start()

            for copy in weight_copies(k):
                copy.wait()
            all_peers(*fwd_args(k)).wait_recv()

            @pl.when(k >= 2)
            def _():
                all_peers(*back_args(k - 2)).wait_send()

            experts_ffn(k)
            send(*back_args(k))
            keep_own(*back_args(k))

        @pl.when(t + 1 < local)
        def _():
            @pl.when(t >= 1)
            def _():
                all_peers(*fwd_args(t - 1)).wait_send()

            dispatch(t + 1)

    for k in range(max(local - 2, 0), local):
        all_peers(*fwd_args(jnp.int32(k))).wait_send()
        all_peers(*back_args(jnp.int32(k))).wait_send()


def solution(mesh):
    n = mesh.shape["ep"]

    def local_layer(tokens, w_gate, expert_ids, keep_second, w_in, w_out):
        _, token_count, model = tokens.shape
        experts = w_gate.shape[1]
        local, _, hidden = w_in.shape
        capacity = 2 * token_count // experts
        rows = n * capacity
        bf16, f32 = jnp.bfloat16, jnp.float32
        sizes = (token_count, model, hidden, experts, local, capacity)
        vmem, hbm = pl.BlockSpec(memory_space=pltpu.VMEM), pl.BlockSpec(memory_space=pl.ANY)
        dma = pltpu.SemaphoreType.DMA
        acc, mix_last, yrecv = pl.pallas_call(
            functools.partial(moe_kernel, n, sizes),
            out_shape=(
                pltpu.VMEM((token_count, model), f32),
                pltpu.VMEM((token_count, rows), bf16),
                pltpu.VMEM((LAG + 1, rows, model), bf16),
            ),
            in_specs=[hbm] * 6,
            out_specs=(vmem, vmem, vmem),
            scratch_shapes=[
                pltpu.VMEM((2, token_count), jnp.int32),
                pltpu.VMEM((1, token_count), jnp.int32),
                pltpu.VMEM((token_count, model), bf16),
                pltpu.VMEM(w_gate.shape, bf16),
                pltpu.VMEM((2, model, hidden), bf16),
                pltpu.VMEM((2, hidden, model), bf16),
                pltpu.VMEM((2, rows, model), bf16),
                pltpu.VMEM((LAG, rows, model), bf16),
                pltpu.VMEM((2, rows, model), bf16),
                pltpu.VMEM((rows, token_count), bf16),
                pltpu.VMEM((rows, hidden), bf16),
                pltpu.VMEM((8, token_count), f32),
                pltpu.VMEM((4, token_count, 128), f32),
                dma((2,)),
                dma((model // TILE,)),
                dma,
                dma((2,)),
                dma((2,)),
                dma((2,)),
                dma((LAG,)),
                dma((2,)),
                dma((LAG + 1,)),
            ],
            compiler_params=pltpu.CompilerParams(
                collective_id=0, has_side_effects=True, vmem_limit_bytes=VMEM_A
            ),
        )(expert_ids[0].T, keep_second, tokens, w_gate, w_in, w_out)
        return pl.pallas_call(
            functools.partial(last_kernel, (local - 1) % (LAG + 1)),
            out_shape=jax.ShapeDtypeStruct(tokens.shape, bf16),
            in_specs=[vmem, vmem, vmem],
            out_specs=hbm,
            scratch_shapes=[pltpu.VMEM((token_count, model), bf16), dma],
            compiler_params=pltpu.CompilerParams(vmem_limit_bytes=VMEM_B),
        )(acc, mix_last, yrecv)

    group_spec = P(("dp", "ep"))
    return jax.shard_map(
        local_layer,
        mesh=mesh,
        in_specs=(group_spec, P(), group_spec, group_spec, P("ep"), P("ep")),
        out_specs=group_spec,
        check_vma=False,
    )
```

```python
import functools

import jax
import jax.numpy as jnp
from jax import lax
from jax.experimental import pallas as pl
from jax.experimental.pallas import tpu as pltpu
from jax.sharding import PartitionSpec as P

MESH = pl.DeviceIdType.MESH
LAG = 3
TILE = 256
PIECE = 256
VMEM_A = 36 * 1024 * 1024
VMEM_B = 12 * 1024 * 1024


def ring_offsets(chip_count):
    return sorted(range(1, chip_count), key=lambda d: -min(d, chip_count - d))


def mix_weights(colb, base, rows, toks):
    base = jnp.int32(base).astype(jnp.float32)
    c1, c2 = colb[0, toks, :] - base, colb[1, toks, :] - base
    w1, w2 = colb[2, toks, :], colb[3, toks, :]
    parts = []
    for lane in range(0, rows, 128):
        want = (lax.broadcasted_iota(jnp.int32, (TILE, 128), 1) + lane).astype(jnp.float32)
        parts.append((jnp.where(c1 == want, w1, 0.0) + jnp.where(c2 == want, w2, 0.0)).astype(jnp.bfloat16))
    return jnp.concatenate(parts, axis=1)


def last_kernel(slot, acc, mix_last, yrecv, out_hbm, stage, sem):
    tokens, model = acc.shape

    width = 2 * TILE

    @pl.loop(0, tokens // TILE)
    def _(i):
        toks = pl.ds(pl.multiple_of(i * TILE, TILE), TILE)
        for j in range(0, model, width):
            cols = pl.ds(j, width)
            got = acc[toks, cols] + jnp.dot(mix_last[toks, :], yrecv[slot, :, cols], preferred_element_type=jnp.float32)
            stage[toks, cols] = got.astype(jnp.bfloat16)
            pltpu.make_async_copy(stage.at[toks, cols], out_hbm.at[0, toks, cols], sem).start()

    pltpu.make_async_copy(stage, out_hbm.at[0], sem).wait()


def moe_kernel(
    n, sizes, ids_hbm, keep_hbm, x_hbm, wg_hbm, win_hbm, wout_hbm,
    acc, mix_last, yrecv,
    ids_ref, keep_ref, x_v, wg_v, win_v, wout_v, fsend, frecv, ysend, dmat, hid, crow, colb,
    id_sem, x_sem, wg_sem, win_sem, wout_sem, fs_sem, fr_sem, ys_sem, yr_sem,
):
    tokens, model, hidden, experts, local, capacity = sizes
    rows = n * capacity
    fslots, yslots = frecv.shape[0], yrecv.shape[0]
    shift = (local - 1).bit_length()
    blocks = tokens // TILE
    me = lax.axis_index("ep")

    def x_copy(j):
        cols = pl.ds(pl.multiple_of(j * TILE, TILE), TILE)
        return pltpu.make_async_copy(x_hbm.at[0, :, cols], x_v.at[:, cols], x_sem.at[j])

    id_copies = (
        pltpu.make_async_copy(ids_hbm, ids_ref, id_sem.at[0]),
        pltpu.make_async_copy(keep_hbm, keep_ref, id_sem.at[1]),
    )
    wg_copy = pltpu.make_async_copy(wg_hbm, wg_v, wg_sem)

    def weight_copies(k):
        b = lax.rem(k, 2)
        return (
            pltpu.make_async_copy(win_hbm.at[k], win_v.at[b], win_sem.at[b]),
            pltpu.make_async_copy(wout_hbm.at[k], wout_v.at[b], wout_sem.at[b]),
        )

    def owner_rows(d):
        return pl.ds(pl.multiple_of(d * capacity, capacity), capacity)

    cores = 2 if n % 2 == 0 else 1
    chips = n // cores
    my_chip, my_core = me // cores, lax.rem(me, cores)
    targets = []
    for dist in ring_offsets(chips) + [0]:
        for c in range(cores):
            if dist == 0 and c == 0:
                continue
            targets.append(lax.rem(my_chip + dist, chips) * cores + lax.rem(my_core + c, cores))

    def send(src, src_slot, dst, dst_slot, s_sem, r_sem, cols=slice(None)):
        for d in targets:
            pltpu.make_async_remote_copy(
                src_ref=src.at[src_slot, owner_rows(d), cols],
                dst_ref=dst.at[dst_slot, owner_rows(me), cols],
                send_sem=s_sem.at[src_slot],
                recv_sem=r_sem.at[dst_slot],
                device_id={"ep": d},
                device_id_type=MESH,
            ).start()

    def all_peers(src, src_slot, dst, dst_slot, s_sem, r_sem):
        part = pl.ds(0, (n - 1) * capacity)
        return pltpu.make_async_remote_copy(
            src_ref=src.at[src_slot, part],
            dst_ref=dst.at[dst_slot, part],
            send_sem=s_sem.at[src_slot],
            recv_sem=r_sem.at[dst_slot],
            device_id={"ep": me},
            device_id_type=MESH,
        )

    def fwd_args(k):
        return (fsend, lax.rem(k, 2), frecv, lax.rem(k, fslots), fs_sem, fr_sem)

    def back_args(k):
        return (ysend, lax.rem(k, 2), yrecv, lax.rem(k, yslots), ys_sem, yr_sem)

    def keep_own(src, src_slot, dst, dst_slot, *_):
        dst[dst_slot, owner_rows(me), :] = src[src_slot, owner_rows(me), :]

    def hot(blk, expert_row):
        return lax.broadcasted_iota(jnp.int32, (experts, TILE), 0) == expert_row

    def load_ids(b):
        cols = pl.ds(b * TILE, TILE)
        return ids_ref[0:1, cols], ids_ref[1:2, cols], keep_ref[0:1, cols] == 1

    def route(on_block):
        bf16, f32 = jnp.bfloat16, jnp.float32
        expert = lax.broadcasted_iota(jnp.int32, (experts, TILE), 0)
        ones = jnp.ones((TILE, 128), bf16)
        order = lax.broadcasted_iota(jnp.int32, (TILE, TILE), 0) < lax.broadcasted_iota(jnp.int32, (TILE, TILE), 1)
        earlier = jnp.concatenate([jnp.where(order, 1.0, 0.0).astype(bf16), ones], axis=1)
        packed_expert = expert.astype(f32).astype(bf16)

        def one_hot(row):
            return jnp.where(packed_expert == row.astype(f32).astype(bf16), bf16(1), bf16(0))

        count = jnp.zeros((experts, TILE), bf16)
        for b in range(blocks):
            count = count + one_hot(load_ids(b)[0])
        base1 = jnp.zeros((experts, 128), f32)
        base2 = jnp.dot(count, ones, preferred_element_type=f32)
        for b in range(blocks):
            on_block(b)
            i1, i2, k2 = load_ids(b)
            kept2 = jnp.where(k2, i2, -1)
            hots = jnp.concatenate([one_hot(i1), one_hot(kept2)], axis=0)
            ahead = jnp.dot(hots, earlier, preferred_element_type=f32)
            ahead1, ahead2 = ahead[:experts], ahead[experts:]
            for lane in range(0, TILE, 128):
                part = slice(lane, lane + 128)
                cols = pl.ds(b * TILE + lane, 128)
                is1, is2 = expert[:, part] == i1[:, part], expert[:, part] == kept2[:, part]
                pos1 = jnp.sum(jnp.where(is1, ahead1[:, part] + base1, 0.0), axis=0, keepdims=True)
                pos2 = jnp.sum(jnp.where(is2, ahead2[:, part] + base2, 0.0), axis=0, keepdims=True)

                def code(e, pos, kept):
                    home = (e & (local - 1)) * rows + (e >> shift) * capacity
                    return jnp.where(kept, home.astype(f32) + pos, -1.0)

                crow[0:1, cols] = code(i1[:, part], pos1, pos1 < capacity)
                crow[1:2, cols] = code(i2[:, part], pos2, jnp.logical_and(k2[:, part], pos2 < capacity))
            base1 = base1 + ahead1[:, TILE:]
            base2 = base2 + ahead2[:, TILE:]

    def gates():
        for b in range(blocks):
            cols = pl.ds(b * TILE, TILE)
            i1, i2, k2 = load_ids(b)
            logits = jnp.dot(x_v[cols, :], wg_v[...], preferred_element_type=jnp.float32).T
            top = jnp.max(logits, axis=0, keepdims=True)
            grown = jnp.exp(logits - top)
            probs = grown / jnp.sum(grown, axis=0, keepdims=True)
            g1 = jnp.sum(jnp.where(hot(b, i1), probs, 0.0), axis=0, keepdims=True)
            g2 = jnp.where(k2, jnp.sum(jnp.where(hot(b, i2), probs, 0.0), axis=0, keepdims=True), 0.0)
            total = g1 + g2
            for q, row in enumerate((crow[0:1, cols], crow[1:2, cols], g1 / total, g2 / total)):
                colb[q, cols, :] = jnp.broadcast_to(row, (128, TILE)).T

    def dispatch_mask(k):
        base = (k * rows).astype(jnp.float32)
        want = lax.broadcasted_iota(jnp.int32, (rows, TILE), 0).astype(jnp.float32).astype(jnp.bfloat16)
        for b in range(blocks):
            cols = pl.ds(b * TILE, TILE)

            def row_of(q):
                row = crow[q : q + 1, cols] - base
                return jnp.where(jnp.logical_and(row >= 0.0, row < rows), row, -1.0).astype(jnp.bfloat16)

            hit = jnp.logical_or(want == row_of(0), want == row_of(1))
            dmat[:, cols] = jnp.where(hit, jnp.bfloat16(1), jnp.bfloat16(0))

    def dispatch_tile(slot, j):
        cols = pl.ds(pl.multiple_of(j * TILE, TILE), TILE)
        fsend[slot, :, cols] = jnp.dot(dmat[...], x_v[:, cols], preferred_element_type=jnp.float32).astype(jnp.bfloat16)

    def dispatch(k):
        dispatch_mask(k)

        @pl.loop(0, model // TILE)
        def _(j):
            dispatch_tile(lax.rem(k, 2), j)

    def experts_ffn(k):
        w, slot, out_slot = lax.rem(k, 2), lax.rem(k, fslots), lax.rem(k, 2)

        @pl.loop(0, hidden // TILE)
        def _(j):
            cols = pl.ds(pl.multiple_of(j * TILE, TILE), TILE)
            h = jnp.dot(frecv[slot], win_v[w, :, cols], preferred_element_type=jnp.float32)
            hid[:, cols] = jnp.maximum(h, 0.0).astype(jnp.bfloat16)

        @pl.loop(0, model // TILE)
        def _(j):
            cols = pl.ds(pl.multiple_of(j * TILE, TILE), TILE)
            y = jnp.dot(hid[...], wout_v[w, :, cols], preferred_element_type=jnp.float32)
            ysend[out_slot, :, cols] = y.astype(jnp.bfloat16)

    def combine(k):
        @pl.loop(0, blocks)
        def _(i):
            toks = pl.ds(pl.multiple_of(i * TILE, TILE), TILE)
            mix = mix_weights(colb, k * rows, rows, toks)
            for j in range(0, model, 2 * TILE):
                cols = pl.ds(j, 2 * TILE)
                acc[toks, cols] += jnp.dot(
                    mix, yrecv[lax.rem(k, yslots), :, cols], preferred_element_type=jnp.float32
                )

    for copy in id_copies:
        copy.start()
    x_copy(0).start()
    barrier = pltpu.get_barrier_semaphore()
    for d in targets:
        pl.semaphore_signal(barrier, inc=1, device_id={"ep": d}, device_id_type=MESH)
    for copy in id_copies:
        copy.wait()
    tiles = model // TILE
    ahead = min(4, tiles - 1)

    def next_tile(b):
        if b % 2 == 0 and 1 + b // 2 <= ahead:
            x_copy(1 + b // 2).start()

    route(next_tile)
    first = jnp.int32(0)
    dispatch_mask(first)
    pl.semaphore_wait(barrier, n - 1)

    @pl.loop(0, model // PIECE)
    def _(piece):
        for j in range(PIECE // TILE):
            tile = piece * (PIECE // TILE) + j
            x_copy(tile).wait()

            @pl.when(tile + ahead + 1 < tiles)
            def _():
                x_copy(tile + ahead + 1).start()

            dispatch_tile(0, tile)
        send(*fwd_args(first), pl.ds(pl.multiple_of(piece * PIECE, PIECE), PIECE))

    keep_own(*fwd_args(first))
    wg_copy.start()
    for copy in weight_copies(first):
        copy.start()

    @pl.loop(0, local + LAG)
    def _(t):
        @pl.when(t >= LAG)
        def _():
            all_peers(*back_args(t - LAG)).wait_recv()

        @pl.when(jnp.logical_and(t >= 1, t < local))
        def _():
            send(*fwd_args(t))
            keep_own(*fwd_args(t))

        @pl.when(t == 1)
        def _():
            wg_copy.wait()
            gates()

            @pl.loop(0, blocks)
            def _(i):
                acc[pl.ds(pl.multiple_of(i * TILE, TILE), TILE), :] = jnp.zeros((TILE, model), jnp.float32)

        @pl.when(jnp.logical_and(t >= LAG, t < local + LAG - 1))
        def _():
            combine(t - LAG)

        @pl.when(t == local)
        def _():
            @pl.loop(0, blocks)
            def _(i):
                toks = pl.ds(pl.multiple_of(i * TILE, TILE), TILE)
                mix_last[toks, :] = mix_weights(colb, (local - 1) * rows, rows, toks)

        @pl.when(jnp.logical_and(t >= 1, t <= local))
        def _():
            k = t - 1

            @pl.when(t < local)
            def _():
                for copy in weight_copies(t):
                    copy.start()

            for copy in weight_copies(k):
                copy.wait()
            all_peers(*fwd_args(k)).wait_recv()

            @pl.when(k >= 2)
            def _():
                all_peers(*back_args(k - 2)).wait_send()

            experts_ffn(k)
            send(*back_args(k))
            keep_own(*back_args(k))

        @pl.when(t + 1 < local)
        def _():
            @pl.when(t >= 1)
            def _():
                all_peers(*fwd_args(t - 1)).wait_send()

            dispatch(t + 1)

    for k in range(max(local - 2, 0), local):
        all_peers(*fwd_args(jnp.int32(k))).wait_send()
        all_peers(*back_args(jnp.int32(k))).wait_send()


def solution(mesh):
    n = mesh.shape["ep"]

    def local_layer(tokens, w_gate, expert_ids, keep_second, w_in, w_out):
        _, token_count, model = tokens.shape
        experts = w_gate.shape[1]
        local, _, hidden = w_in.shape
        capacity = 2 * token_count // experts
        rows = n * capacity
        bf16, f32 = jnp.bfloat16, jnp.float32
        sizes = (token_count, model, hidden, experts, local, capacity)
        vmem, hbm = pl.BlockSpec(memory_space=pltpu.VMEM), pl.BlockSpec(memory_space=pl.ANY)
        dma = pltpu.SemaphoreType.DMA
        acc, mix_last, yrecv = pl.pallas_call(
            functools.partial(moe_kernel, n, sizes),
            out_shape=(
                pltpu.VMEM((token_count, model), f32),
                pltpu.VMEM((token_count, rows), bf16),
                pltpu.VMEM((LAG + 1, rows, model), bf16),
            ),
            in_specs=[hbm] * 6,
            out_specs=(vmem, vmem, vmem),
            scratch_shapes=[
                pltpu.VMEM((2, token_count), jnp.int32),
                pltpu.VMEM((1, token_count), jnp.int32),
                pltpu.VMEM((token_count, model), bf16),
                pltpu.VMEM(w_gate.shape, bf16),
                pltpu.VMEM((2, model, hidden), bf16),
                pltpu.VMEM((2, hidden, model), bf16),
                pltpu.VMEM((2, rows, model), bf16),
                pltpu.VMEM((LAG, rows, model), bf16),
                pltpu.VMEM((2, rows, model), bf16),
                pltpu.VMEM((rows, token_count), bf16),
                pltpu.VMEM((rows, hidden), bf16),
                pltpu.VMEM((8, token_count), f32),
                pltpu.VMEM((4, token_count, 128), f32),
                dma((2,)),
                dma((model // TILE,)),
                dma,
                dma((2,)),
                dma((2,)),
                dma((2,)),
                dma((LAG,)),
                dma((2,)),
                dma((LAG + 1,)),
            ],
            compiler_params=pltpu.CompilerParams(
                collective_id=0, has_side_effects=True, vmem_limit_bytes=VMEM_A
            ),
        )(expert_ids[0].T, keep_second, tokens, w_gate, w_in, w_out)
        return pl.pallas_call(
            functools.partial(last_kernel, (local - 1) % (LAG + 1)),
            out_shape=jax.ShapeDtypeStruct(tokens.shape, bf16),
            in_specs=[vmem, vmem, vmem],
            out_specs=hbm,
            scratch_shapes=[pltpu.VMEM((token_count, model), bf16), dma],
            compiler_params=pltpu.CompilerParams(vmem_limit_bytes=VMEM_B),
        )(acc, mix_last, yrecv)

    group_spec = P(("dp", "ep"))
    return jax.shard_map(
        local_layer,
        mesh=mesh,
        in_specs=(group_spec, P(), group_spec, group_spec, P("ep"), P("ep")),
        out_specs=group_spec,
        check_vma=False,
    )
```

```python
import functools

import jax
import jax.numpy as jnp
from jax import lax
from jax.experimental import pallas as pl
from jax.experimental.pallas import tpu as pltpu
from jax.sharding import PartitionSpec as P

MESH = pl.DeviceIdType.MESH
LAG = 3
TILE = 256
PIECE = 256
VMEM_A = 36 * 1024 * 1024
VMEM_B = 12 * 1024 * 1024


def ring_offsets(chip_count):
    return sorted(range(1, chip_count), key=lambda d: -min(d, chip_count - d))


def mix_weights(colb, base, rows, toks):
    base = jnp.int32(base).astype(jnp.float32)
    c1, c2 = colb[0, toks, :] - base, colb[1, toks, :] - base
    w1, w2 = colb[2, toks, :], colb[3, toks, :]
    parts = []
    for lane in range(0, rows, 128):
        want = (lax.broadcasted_iota(jnp.int32, (TILE, 128), 1) + lane).astype(jnp.float32)
        parts.append((jnp.where(c1 == want, w1, 0.0) + jnp.where(c2 == want, w2, 0.0)).astype(jnp.bfloat16))
    return jnp.concatenate(parts, axis=1)


def last_kernel(slot, acc, mix_last, yrecv, out_hbm, stage, sem):
    tokens, model = acc.shape

    width = 2 * TILE

    @pl.loop(0, tokens // TILE)
    def _(i):
        toks = pl.ds(pl.multiple_of(i * TILE, TILE), TILE)
        for j in range(0, model, width):
            cols = pl.ds(j, width)
            got = acc[toks, cols]
            if j >= model // 2:
                got += jnp.dot(mix_last[toks, :], yrecv[slot, :, cols], preferred_element_type=jnp.float32)
            stage[toks, cols] = got.astype(jnp.bfloat16)
            pltpu.make_async_copy(stage.at[toks, cols], out_hbm.at[0, toks, cols], sem).start()

    pltpu.make_async_copy(stage, out_hbm.at[0], sem).wait()


def moe_kernel(
    n, sizes, ids_hbm, keep_hbm, x_hbm, wg_hbm, win_hbm, wout_hbm,
    acc, mix_last, yrecv,
    ids_ref, keep_ref, x_v, wg_v, win_v, wout_v, fsend, frecv, ysend, dmat, hid, crow, colb,
    id_sem, x_sem, wg_sem, win_sem, wout_sem, fs_sem, fr_sem, ys_sem, yr_sem,
):
    tokens, model, hidden, experts, local, capacity = sizes
    rows = n * capacity
    fslots, yslots = frecv.shape[0], yrecv.shape[0]
    shift = (local - 1).bit_length()
    blocks = tokens // TILE
    me = lax.axis_index("ep")

    def x_copy(j):
        cols = pl.ds(pl.multiple_of(j * TILE, TILE), TILE)
        return pltpu.make_async_copy(x_hbm.at[0, :, cols], x_v.at[:, cols], x_sem.at[j])

    id_copies = (
        pltpu.make_async_copy(ids_hbm, ids_ref, id_sem.at[0]),
        pltpu.make_async_copy(keep_hbm, keep_ref, id_sem.at[1]),
    )
    wg_copy = pltpu.make_async_copy(wg_hbm, wg_v, wg_sem)

    def weight_copies(k):
        b = lax.rem(k, 2)
        return (
            pltpu.make_async_copy(win_hbm.at[k], win_v.at[b], win_sem.at[b]),
            pltpu.make_async_copy(wout_hbm.at[k], wout_v.at[b], wout_sem.at[b]),
        )

    def owner_rows(d):
        return pl.ds(pl.multiple_of(d * capacity, capacity), capacity)

    cores = 2 if n % 2 == 0 else 1
    chips = n // cores
    my_chip, my_core = me // cores, lax.rem(me, cores)
    targets = []
    for dist in ring_offsets(chips) + [0]:
        for c in range(cores):
            if dist == 0 and c == 0:
                continue
            targets.append(lax.rem(my_chip + dist, chips) * cores + lax.rem(my_core + c, cores))

    def send(src, src_slot, dst, dst_slot, s_sem, r_sem, cols=slice(None), own_sem=None):
        for d in targets:
            pltpu.make_async_remote_copy(
                src_ref=src.at[src_slot, owner_rows(d), cols],
                dst_ref=dst.at[dst_slot, owner_rows(me), cols],
                send_sem=s_sem.at[src_slot if own_sem is None else own_sem[0]],
                recv_sem=r_sem.at[dst_slot if own_sem is None else own_sem[1]],
                device_id={"ep": d},
                device_id_type=MESH,
            ).start()

    def all_peers(src, src_slot, dst, dst_slot, s_sem, r_sem, cols=slice(None), own_sem=None):
        part = pl.ds(0, (n - 1) * capacity)
        return pltpu.make_async_remote_copy(
            src_ref=src.at[src_slot, part, cols],
            dst_ref=dst.at[dst_slot, part, cols],
            send_sem=s_sem.at[src_slot if own_sem is None else own_sem[0]],
            recv_sem=r_sem.at[dst_slot if own_sem is None else own_sem[1]],
            device_id={"ep": me},
            device_id_type=MESH,
        )

    def fwd_args(k):
        return (fsend, lax.rem(k, 2), frecv, lax.rem(k, fslots), fs_sem, fr_sem)

    def back_args(k):
        return (ysend, lax.rem(k, 2), yrecv, lax.rem(k, yslots), ys_sem, yr_sem)

    half = model // 2
    last_halves = (
        (*back_args(jnp.int32(local - 1)), pl.ds(0, half)),
        (*back_args(jnp.int32(local - 1)), pl.ds(half, half), (ys_sem.shape[0] - 1, yslots)),
    )

    def keep_own(src, src_slot, dst, dst_slot, *_):
        dst[dst_slot, owner_rows(me), :] = src[src_slot, owner_rows(me), :]

    def hot(blk, expert_row):
        return lax.broadcasted_iota(jnp.int32, (experts, TILE), 0) == expert_row

    def load_ids(b):
        cols = pl.ds(b * TILE, TILE)
        return ids_ref[0:1, cols], ids_ref[1:2, cols], keep_ref[0:1, cols] == 1

    def route(on_block):
        bf16, f32 = jnp.bfloat16, jnp.float32
        expert = lax.broadcasted_iota(jnp.int32, (experts, TILE), 0)
        ones = jnp.ones((TILE, 128), bf16)
        order = lax.broadcasted_iota(jnp.int32, (TILE, TILE), 0) < lax.broadcasted_iota(jnp.int32, (TILE, TILE), 1)
        earlier = jnp.concatenate([jnp.where(order, 1.0, 0.0).astype(bf16), ones], axis=1)
        packed_expert = expert.astype(f32).astype(bf16)

        def one_hot(row):
            return jnp.where(packed_expert == row.astype(f32).astype(bf16), bf16(1), bf16(0))

        count = jnp.zeros((experts, TILE), bf16)
        for b in range(blocks):
            count = count + one_hot(load_ids(b)[0])
        base1 = jnp.zeros((experts, 128), f32)
        base2 = jnp.dot(count, ones, preferred_element_type=f32)
        for b in range(blocks):
            on_block(b)
            i1, i2, k2 = load_ids(b)
            kept2 = jnp.where(k2, i2, -1)
            hots = jnp.concatenate([one_hot(i1), one_hot(kept2)], axis=0)
            ahead = jnp.dot(hots, earlier, preferred_element_type=f32)
            ahead1, ahead2 = ahead[:experts], ahead[experts:]
            for lane in range(0, TILE, 128):
                part = slice(lane, lane + 128)
                cols = pl.ds(b * TILE + lane, 128)
                is1, is2 = expert[:, part] == i1[:, part], expert[:, part] == kept2[:, part]
                pos1 = jnp.sum(jnp.where(is1, ahead1[:, part] + base1, 0.0), axis=0, keepdims=True)
                pos2 = jnp.sum(jnp.where(is2, ahead2[:, part] + base2, 0.0), axis=0, keepdims=True)

                def code(e, pos, kept):
                    home = (e & (local - 1)) * rows + (e >> shift) * capacity
                    return jnp.where(kept, home.astype(f32) + pos, -1.0)

                crow[0:1, cols] = code(i1[:, part], pos1, pos1 < capacity)
                crow[1:2, cols] = code(i2[:, part], pos2, jnp.logical_and(k2[:, part], pos2 < capacity))
            base1 = base1 + ahead1[:, TILE:]
            base2 = base2 + ahead2[:, TILE:]

    def gates():
        for b in range(blocks):
            cols = pl.ds(b * TILE, TILE)
            i1, i2, k2 = load_ids(b)
            logits = jnp.dot(x_v[cols, :], wg_v[...], preferred_element_type=jnp.float32).T
            top = jnp.max(logits, axis=0, keepdims=True)
            grown = jnp.exp(logits - top)
            probs = grown / jnp.sum(grown, axis=0, keepdims=True)
            g1 = jnp.sum(jnp.where(hot(b, i1), probs, 0.0), axis=0, keepdims=True)
            g2 = jnp.where(k2, jnp.sum(jnp.where(hot(b, i2), probs, 0.0), axis=0, keepdims=True), 0.0)
            total = g1 + g2
            for q, row in enumerate((crow[0:1, cols], crow[1:2, cols], g1 / total, g2 / total)):
                colb[q, cols, :] = jnp.broadcast_to(row, (128, TILE)).T

    def dispatch_mask(k):
        base = (k * rows).astype(jnp.float32)
        want = lax.broadcasted_iota(jnp.int32, (rows, TILE), 0).astype(jnp.float32).astype(jnp.bfloat16)
        for b in range(blocks):
            cols = pl.ds(b * TILE, TILE)

            def row_of(q):
                row = crow[q : q + 1, cols] - base
                return jnp.where(jnp.logical_and(row >= 0.0, row < rows), row, -1.0).astype(jnp.bfloat16)

            hit = jnp.logical_or(want == row_of(0), want == row_of(1))
            dmat[:, cols] = jnp.where(hit, jnp.bfloat16(1), jnp.bfloat16(0))

    def dispatch_tile(slot, j):
        cols = pl.ds(pl.multiple_of(j * TILE, TILE), TILE)
        fsend[slot, :, cols] = jnp.dot(dmat[...], x_v[:, cols], preferred_element_type=jnp.float32).astype(jnp.bfloat16)

    def dispatch(k):
        dispatch_mask(k)

        @pl.loop(0, model // TILE)
        def _(j):
            dispatch_tile(lax.rem(k, 2), j)

    def experts_ffn(k):
        w, slot, out_slot = lax.rem(k, 2), lax.rem(k, fslots), lax.rem(k, 2)

        @pl.loop(0, hidden // TILE)
        def _(j):
            cols = pl.ds(pl.multiple_of(j * TILE, TILE), TILE)
            h = jnp.dot(frecv[slot], win_v[w, :, cols], preferred_element_type=jnp.float32)
            hid[:, cols] = jnp.maximum(h, 0.0).astype(jnp.bfloat16)

        for h in range(2):

            @pl.loop(h * half // TILE, (h + 1) * half // TILE)
            def _(j):
                cols = pl.ds(pl.multiple_of(j * TILE, TILE), TILE)
                y = jnp.dot(hid[...], wout_v[w, :, cols], preferred_element_type=jnp.float32)
                ysend[out_slot, :, cols] = y.astype(jnp.bfloat16)

            @pl.when(k == local - 1)
            def _():
                send(*last_halves[h])

        @pl.when(k < local - 1)
        def _():
            send(*back_args(k))

    def combine(k):
        @pl.loop(0, blocks)
        def _(i):
            toks = pl.ds(pl.multiple_of(i * TILE, TILE), TILE)
            mix = mix_weights(colb, k * rows, rows, toks)
            for j in range(0, model, 2 * TILE):
                cols = pl.ds(j, 2 * TILE)
                acc[toks, cols] += jnp.dot(
                    mix, yrecv[lax.rem(k, yslots), :, cols], preferred_element_type=jnp.float32
                )

    for copy in id_copies:
        copy.start()
    x_copy(0).start()
    barrier = pltpu.get_barrier_semaphore()
    for d in targets:
        pl.semaphore_signal(barrier, inc=1, device_id={"ep": d}, device_id_type=MESH)
    for copy in id_copies:
        copy.wait()
    tiles = model // TILE
    ahead = min(4, tiles - 1)

    def next_tile(b):
        if b % 2 == 0 and 1 + b // 2 <= ahead:
            x_copy(1 + b // 2).start()

    route(next_tile)
    first = jnp.int32(0)
    dispatch_mask(first)
    pl.semaphore_wait(barrier, n - 1)

    @pl.loop(0, model // PIECE)
    def _(piece):
        for j in range(PIECE // TILE):
            tile = piece * (PIECE // TILE) + j
            x_copy(tile).wait()

            @pl.when(tile + ahead + 1 < tiles)
            def _():
                x_copy(tile + ahead + 1).start()

            dispatch_tile(0, tile)
        send(*fwd_args(first), pl.ds(pl.multiple_of(piece * PIECE, PIECE), PIECE))

    keep_own(*fwd_args(first))
    wg_copy.start()
    for copy in weight_copies(first):
        copy.start()

    @pl.loop(0, local + LAG - 1)
    def _(t):
        @pl.when(t >= LAG)
        def _():
            all_peers(*back_args(t - LAG)).wait_recv()

        @pl.when(jnp.logical_and(t >= 1, t < local))
        def _():
            send(*fwd_args(t))
            keep_own(*fwd_args(t))

        @pl.when(t == 1)
        def _():
            wg_copy.wait()
            gates()

            @pl.loop(0, blocks)
            def _(i):
                acc[pl.ds(pl.multiple_of(i * TILE, TILE), TILE), :] = jnp.zeros((TILE, model), jnp.float32)

        @pl.when(t >= LAG)
        def _():
            combine(t - LAG)

        @pl.when(t == local)
        def _():
            @pl.loop(0, blocks)
            def _(i):
                toks = pl.ds(pl.multiple_of(i * TILE, TILE), TILE)
                mix_last[toks, :] = mix_weights(colb, (local - 1) * rows, rows, toks)

        @pl.when(jnp.logical_and(t >= 1, t <= local))
        def _():
            k = t - 1

            @pl.when(t < local)
            def _():
                for copy in weight_copies(t):
                    copy.start()

            for copy in weight_copies(k):
                copy.wait()
            all_peers(*fwd_args(k)).wait_recv()

            @pl.when(k >= 2)
            def _():
                all_peers(*back_args(k - 2)).wait_send()

            experts_ffn(k)
            keep_own(*back_args(k))

        @pl.when(t + 1 < local)
        def _():
            @pl.when(t >= 1)
            def _():
                all_peers(*fwd_args(t - 1)).wait_send()

            dispatch(t + 1)

    all_peers(*last_halves[0]).wait_recv()

    @pl.loop(0, blocks)
    def _(i):
        toks = pl.ds(pl.multiple_of(i * TILE, TILE), TILE)
        for j in range(0, half, 2 * TILE):
            cols = pl.ds(j, 2 * TILE)
            acc[toks, cols] += jnp.dot(
                mix_last[toks, :], yrecv[(local - 1) % yslots, :, cols], preferred_element_type=jnp.float32
            )

    all_peers(*last_halves[1]).wait_recv()
    for k in range(max(local - 2, 0), local):
        all_peers(*fwd_args(jnp.int32(k))).wait_send()
    all_peers(*back_args(jnp.int32(local - 2))).wait_send()
    for part in last_halves:
        all_peers(*part).wait_send()


def solution(mesh):
    n = mesh.shape["ep"]

    def local_layer(tokens, w_gate, expert_ids, keep_second, w_in, w_out):
        _, token_count, model = tokens.shape
        experts = w_gate.shape[1]
        local, _, hidden = w_in.shape
        capacity = 2 * token_count // experts
        rows = n * capacity
        bf16, f32 = jnp.bfloat16, jnp.float32
        sizes = (token_count, model, hidden, experts, local, capacity)
        vmem, hbm = pl.BlockSpec(memory_space=pltpu.VMEM), pl.BlockSpec(memory_space=pl.ANY)
        dma = pltpu.SemaphoreType.DMA
        acc, mix_last, yrecv = pl.pallas_call(
            functools.partial(moe_kernel, n, sizes),
            out_shape=(
                pltpu.VMEM((token_count, model), f32),
                pltpu.VMEM((token_count, rows), bf16),
                pltpu.VMEM((LAG + 1, rows, model), bf16),
            ),
            in_specs=[hbm] * 6,
            out_specs=(vmem, vmem, vmem),
            scratch_shapes=[
                pltpu.VMEM((2, token_count), jnp.int32),
                pltpu.VMEM((1, token_count), jnp.int32),
                pltpu.VMEM((token_count, model), bf16),
                pltpu.VMEM(w_gate.shape, bf16),
                pltpu.VMEM((2, model, hidden), bf16),
                pltpu.VMEM((2, hidden, model), bf16),
                pltpu.VMEM((2, rows, model), bf16),
                pltpu.VMEM((LAG, rows, model), bf16),
                pltpu.VMEM((2, rows, model), bf16),
                pltpu.VMEM((rows, token_count), bf16),
                pltpu.VMEM((rows, hidden), bf16),
                pltpu.VMEM((8, token_count), f32),
                pltpu.VMEM((4, token_count, 128), f32),
                dma((2,)),
                dma((model // TILE,)),
                dma,
                dma((2,)),
                dma((2,)),
                dma((2,)),
                dma((LAG,)),
                dma((3,)),
                dma((LAG + 2,)),
            ],
            compiler_params=pltpu.CompilerParams(
                collective_id=0, has_side_effects=True, vmem_limit_bytes=VMEM_A
            ),
        )(expert_ids[0].T, keep_second, tokens, w_gate, w_in, w_out)
        return pl.pallas_call(
            functools.partial(last_kernel, (local - 1) % (LAG + 1)),
            out_shape=jax.ShapeDtypeStruct(tokens.shape, bf16),
            in_specs=[vmem, vmem, vmem],
            out_specs=hbm,
            scratch_shapes=[pltpu.VMEM((token_count, model), bf16), dma],
            compiler_params=pltpu.CompilerParams(vmem_limit_bytes=VMEM_B),
        )(acc, mix_last, yrecv)

    group_spec = P(("dp", "ep"))
    return jax.shard_map(
        local_layer,
        mesh=mesh,
        in_specs=(group_spec, P(), group_spec, group_spec, P("ep"), P("ep")),
        out_specs=group_spec,
        check_vma=False,
    )
```
